128 devices in a mesh: grp: 4 (over y), col: 32 (over z, x, core).
Axes of the slice: x: 4, y: 4, z: 4, core: 2. Of those that a mesh axis runs over, the one named last changes fastest.
Arguments:
- start_block: float32 [16, 32768], P(None, ('grp', 'col')), may hold values from -6 to 6
- tile_values: float32 [4, 32, 32, 256, 256], P('grp', 'col'), may hold values from 0 to 1, as said below
- tile_row: int32 [4, 32, 32], P('grp', 'col'), may hold values from 0 to 127, as said below
- tile_col: int32 [4, 32, 32], P('grp', 'col'), may hold values from 0 to 127, as said below
- tile_count: int32 [4, 32], P('grp', 'col'), may hold values from 8 to 32, as said below
Outputs:
- basis: float32 [5, 16, 32768], P(None, None, ('grp', 'col'))
- projections: float32 [4, 4, 16, 16], replicated
- factors: float32 [5, 16, 16], replicated
The draws below stay inside these ranges and needn't reach their ends.
Inputs may be any that keep to these rules, and one draw needn't show every extreme that they name: `tile_row`: A tile of the device at grp index g lies in tile rows g * 32 * 1 to (g + 1) * 32 - 1. `tile_col`: A tile column t of the device at col index c has (t) % 32 == c. Coordinate pairs may repeat; repeated tiles add. The live tiles of a device are its first tile_count slots; some device has all 32 slots live. `tile_values`: entries are nonnegative.
All inputs are finite; a program needn't handle non-finite values.
Results may differ from the reference program's by a relative error of at most 0.0003.
Values sent between devices are 32-bit elements; how exact they have to be, the bound alone decides.
No kernel may reach another device: no remote copies, remote signals or barrier semaphores. Data moves between devices by JAX's collectives and lax.ppermute only.
A program may use at most 64 MiB of HBM per device.

```python
import math
import jax
import jax.numpy as jnp
from jax import lax

TILE = 256
BLOCK = 16
ITERS = 4
ROW_TILES = 1
SLOTS = 32
NODES = 32768
N_GRP = 4
N_COL = 32


def draw_tile_row(key, part):
    offsets = jax.random.randint(jax.random.fold_in(key, 11), (N_GRP, N_COL, SLOTS), 0, N_COL * ROW_TILES, dtype=jnp.int32)
    groups = jnp.arange(N_GRP, dtype=jnp.int32)[:, None, None]
    return groups * (N_COL * ROW_TILES) + offsets


def draw_tile_col(key, part):
    group_pick = jax.random.randint(jax.random.fold_in(key, 21), (N_GRP, N_COL, SLOTS), 0, N_GRP, dtype=jnp.int32)
    within = jax.random.randint(jax.random.fold_in(key, 22), (N_GRP, N_COL, SLOTS), 0, ROW_TILES, dtype=jnp.int32)
    columns = jnp.arange(N_COL, dtype=jnp.int32)[None, :, None]
    return (group_pick * N_COL + columns) * ROW_TILES + within


def draw_tile_count(key, part):
    counts = jax.random.randint(jax.random.fold_in(key, 31), (N_GRP, N_COL), max(1, SLOTS // 4), SLOTS + 1, dtype=jnp.int32)
    chosen = jax.random.randint(jax.random.fold_in(key, 32), (), 0, N_GRP * N_COL, dtype=jnp.int32)
    flat_index = jnp.arange(N_GRP * N_COL, dtype=jnp.int32).reshape(N_GRP, N_COL)
    return jnp.where(flat_index == chosen, SLOTS, counts).astype(jnp.int32)


def draw_tile_values(key, part):
    array_shape = (N_GRP, N_COL, SLOTS, TILE, TILE)
    lowest = 0.1
    entries = jax.random.uniform(jax.random.fold_in(key, 41), array_shape, jnp.float32)
    row_scale = jnp.exp(jax.random.uniform(jax.random.fold_in(key, 42), (N_GRP, N_COL, SLOTS, TILE, 1), jnp.float32, math.log(lowest), 0.0))
    col_scale = jnp.exp(jax.random.uniform(jax.random.fold_in(key, 43), (N_GRP, N_COL, SLOTS, 1, TILE), jnp.float32, math.log(lowest), 0.0))
    return entries * row_scale * col_scale * (20.0 * ROW_TILES / (SLOTS * TILE))


def block_scale(stream_key, shape, cuts, low, largest):
    level = 1.0
    for axis_at, blocks in cuts:
        draws = jax.random.uniform(jax.random.fold_in(jax.random.fold_in(stream_key, 6), axis_at), (blocks,), jnp.float32, low / len(cuts), largest / len(cuts))
        level = level * jnp.repeat(jnp.exp(draws), shape[axis_at] // blocks).reshape((-1,) + (1,) * (len(shape) - 1 - axis_at))
    return level


def noise(key, dims, deviation, limit, cuts=(), held_as=jnp.bfloat16):
    drawn = deviation * jax.random.normal(key, dims, jnp.float32)
    if cuts:
        drawn = drawn * block_scale(key, dims, cuts, -0.22, 0.18)
    return jnp.clip(drawn, -limit, limit).astype(held_as)


def setup_inputs(seed: int = 0) -> dict:
    splits = jax.random.split(jax.random.key(seed), 6)
    start_block = noise(splits[0], (BLOCK, NODES), 1.0, 6.0, ((1, 128),), jnp.float32)
    tile_values = draw_tile_values(jax.random.fold_in(splits[5], 71), 0)
    tile_row = draw_tile_row(jax.random.fold_in(splits[5], 71), 0)
    tile_col = draw_tile_col(jax.random.fold_in(splits[5], 71), 0)
    tile_count = draw_tile_count(jax.random.fold_in(splits[5], 71), 0)
    return {"start_block": start_block, "tile_values": tile_values, "tile_row": tile_row, "tile_col": tile_col, "tile_count": tile_count}


highest = lax.Precision.HIGHEST

def apply_weights(vector, flat_tiles, flat_rows, flat_cols, flat_live):

    def visit_tile(running, scan_item):
        tile_block, row_tile, col_tile, weight = scan_item
        row_start = (row_tile * TILE).astype(jnp.int32)
        col_start = (col_tile * TILE).astype(jnp.int32)
        col_piece = lax.dynamic_slice_in_dim(vector, col_start, TILE, 1)
        row_piece = lax.dynamic_slice_in_dim(vector, row_start, TILE, 1)
        into_rows = jnp.dot(col_piece, tile_block.T, precision=highest) * weight
        into_cols = jnp.dot(row_piece, tile_block, precision=highest) * weight
        current = lax.dynamic_slice_in_dim(running, row_start, TILE, 1)
        running = lax.dynamic_update_slice_in_dim(running, current + into_rows, row_start, 1)
        current = lax.dynamic_slice_in_dim(running, col_start, TILE, 1)
        running = lax.dynamic_update_slice_in_dim(running, current + into_cols, col_start, 1)
        return (running, None)
    initial = jnp.zeros(vector.shape, jnp.float32)
    result, unused = lax.scan(visit_tile, initial, (flat_tiles, flat_rows, flat_cols, flat_live))
    return result

def orthonormal(block_rows):
    gram_now = jnp.dot(block_rows, block_rows.T, precision=highest) / NODES
    factor = jnp.linalg.cholesky(gram_now)
    solved = jax.scipy.linalg.solve_triangular(factor, block_rows, lower=True)
    return (solved, factor)

def reference(start_block, tile_values, tile_row, tile_col, tile_count):
    flat_tiles = tile_values.reshape(-1, TILE, TILE)
    flat_rows = tile_row.reshape(-1).astype(jnp.int32)
    flat_cols = tile_col.reshape(-1).astype(jnp.int32)
    live_mask = jnp.arange(SLOTS, dtype=jnp.int32)[None, None, :] < tile_count[:, :, None]
    flat_live = live_mask.reshape(-1).astype(jnp.float32)
    ones_row = jnp.ones((1, NODES), jnp.float32)
    degree = apply_weights(ones_row, flat_tiles, flat_rows, flat_cols, flat_live)

    def laplace(vector):
        return degree * vector - apply_weights(vector, flat_tiles, flat_rows, flat_cols, flat_live)
    first_block, factor = orthonormal(start_block)
    basis_list = [first_block]
    factor_list = [factor]
    projections = jnp.zeros((ITERS, ITERS, BLOCK, BLOCK), jnp.float32)
    for step_index in range(ITERS):
        applied = laplace(basis_list[-1])
        stacked = jnp.stack(basis_list)
        coeffs = jnp.einsum('an,jbn->jab', applied, stacked, precision=highest) / NODES
        applied = applied - jnp.einsum('jab,jbn->an', coeffs, stacked, precision=highest)
        next_block, factor = orthonormal(applied)
        basis_list.append(next_block)
        factor_list.append(factor)
        projections = projections.at[step_index, :step_index + 1].set(coeffs)
    return (jnp.stack(basis_list), projections, jnp.stack(factor_list))
```

```python
import functools
import jax
import jax.numpy as jnp
from jax import lax
from jax.experimental import pallas as pl
from jax.experimental.pallas import tpu as pltpu
from jax.sharding import Mesh
from jax.sharding import PartitionSpec as P

ITERS = 4
ZX = ("col_0", "col_1")
CORE = "col_2"
GRP_COL = ("grp", "col_0", "col_1", "col_2")
GROUP = 4
highest = lax.Precision.HIGHEST
VMEM = pl.BlockSpec(memory_space=pltpu.VMEM)
SMEM = pl.BlockSpec(memory_space=pltpu.SMEM)
HBM = pl.BlockSpec(memory_space=pl.ANY)
f32 = jnp.float32
bf16 = jnp.bfloat16


def split(x):
    hi = x.astype(bf16)
    return hi, (x - hi.astype(f32)).astype(bf16)


def dot(a, b, dims):
    return lax.dot_general(a, b, (dims, ((), ())), preferred_element_type=f32)


def dot_f32(a, b, dims):
    return lax.dot_general(a, b, (dims, ((), ())), precision=highest, preferred_element_type=f32)


def tile_copies(tiles, buf, sems):
    slots = buf.shape[0]
    return [
        pltpu.make_async_copy(
            tiles.at[0, 0, pl.ds(q * GROUP, GROUP)], buf.at[pl.ds(q * GROUP, GROUP)], sems.at[q]
        )
        for q in range(slots // GROUP)
    ]


def products(lhs_hi, lhs_lo, tile, dims, first):
    hi, lo = split(tile)
    top = dot(lhs_hi, hi, dims)
    low = dot(lhs_lo, lo, dims)
    out = top[0:16] + top[16:32] + low[0:16]
    if first:
        out = jnp.concatenate([out, top[32:40] + low[16:24]], axis=0)
    return out


def stacked_lhs(piece, first):
    hi, lo = split(piece)
    if first:
        ones = jnp.ones((16, piece.shape[1]), bf16)
        return jnp.concatenate([hi, lo, ones], axis=0), jnp.concatenate([hi, ones], axis=0)
    return jnp.concatenate([hi, lo], axis=0), hi


def rows_kernel(first, info, tiles, own, one, two, three, mine, other, buf, lhs_hi, lhs_lo, sems):
    copies = tile_copies(tiles, buf, sems)
    for copy in copies:
        copy.start()
    for k, piece in enumerate((own, one, two, three)):
        lhs_hi[k], lhs_lo[k] = stacked_lhs(piece[0:16], first)
    mine[...] = jnp.zeros_like(mine)
    other[...] = jnp.zeros_like(other)
    for q, copy in enumerate(copies):
        copy.wait()

        @pl.when(q * GROUP < info[4, 0])
        def _():
            results = []
            for u in range(GROUP):
                s = q * GROUP + u
                k = info[2, s]
                results.append(
                    products(lhs_hi[k], lhs_lo[k], buf[s], ((1,), (1,)), first)
                    * (s < info[4, 0]).astype(f32)
                )
            for u in range(GROUP):
                s = q * GROUP + u

                @pl.when(info[1, s] == 0)
                def _():
                    mine[info[0, s]] += results[u]

                @pl.when(info[1, s] != 0)
                def _():
                    other[info[0, s]] += results[u]


def cols_kernel(first, info, tiles, near, far, own, one, two, three, buf, acc, sems):
    copies = tile_copies(tiles, buf, sems)
    for copy in copies:
        copy.start()
    acc[...] = jnp.zeros_like(acc)
    gram = jnp.zeros_like(near[0, 16:24])
    for p in range(near.shape[0]):
        gram = gram + (near[p, 16:24] + far[p, 16:24])
    for q, copy in enumerate(copies):
        copy.wait()

        @pl.when(q * GROUP < info[4, 0])
        def _():
            results = []
            for u in range(GROUP):
                s = q * GROUP + u
                place = info[0, s]
                piece = jnp.where(info[1, s] == 0, near[place, 0:16], far[place, 0:16])
                left_hi, left_lo = stacked_lhs(piece, first)
                results.append(
                    products(left_hi, left_lo, buf[s], ((1,), (0,)), first)
                    * (s < info[4, 0]).astype(f32)
                )
            for u in range(GROUP):
                s = q * GROUP + u
                acc[info[3, s]] += results[u]

    for k, out in enumerate((own, one, two, three)):
        out[...] = jnp.concatenate([acc[k], gram], axis=0)


def rows_product(first, info, tiles, pieces):
    height = 24 if first else 16
    slots, size = tiles.shape[2], tiles.shape[3]
    out = jax.ShapeDtypeStruct((16, height, size), f32)
    return pl.pallas_call(
        functools.partial(rows_kernel, first),
        name="rows_first" if first else "rows_next",
        out_shape=(out, out),
        in_specs=[SMEM, HBM] + [VMEM] * 4,
        out_specs=(VMEM, VMEM),
        scratch_shapes=[
            pltpu.VMEM((slots, size, size), f32),
            pltpu.VMEM((4, 48 if first else 32, size), bf16),
            pltpu.VMEM((4, 32 if first else 16, size), bf16),
            pltpu.SemaphoreType.DMA((slots // GROUP,)),
        ],
        cost_estimate=pl.CostEstimate(flops=400_000_000, bytes_accessed=8 << 20, transcendentals=0),
    )(info, tiles, *pieces)


def cols_product(first, info, tiles, near, far):
    height = 24 if first else 16
    slots, size = tiles.shape[2], tiles.shape[3]
    out = jax.ShapeDtypeStruct((height + 8, size), f32)
    return pl.pallas_call(
        functools.partial(cols_kernel, first),
        name="cols_first" if first else "cols_next",
        out_shape=(out,) * 4,
        in_specs=[SMEM, HBM, VMEM, VMEM],
        out_specs=(VMEM,) * 4,
        scratch_shapes=[
            pltpu.VMEM((slots, size, size), f32),
            pltpu.VMEM((4, height, size), f32),
            pltpu.SemaphoreType.DMA((slots // GROUP,)),
        ],
        cost_estimate=pl.CostEstimate(flops=400_000_000, bytes_accessed=8 << 20, transcendentals=0),
    )(info, tiles, near, far)


def unpack_gram(packed):
    return jnp.concatenate([packed[:, 0:128], packed[:, 128:256]], axis=0)


def pack_gram(gram):
    width = gram.shape[1]
    if width < 128:
        gram = jnp.concatenate([gram, jnp.zeros((16, 128 - width), f32)], axis=1)
    return jnp.concatenate([gram[0:8], gram[8:16]], axis=1)


def eye16():
    return (
        lax.broadcasted_iota(jnp.int32, (16, 16), 0) == lax.broadcasted_iota(jnp.int32, (16, 16), 1)
    ).astype(f32)


def factor_and_inverse(gram):
    work = jnp.concatenate([gram, eye16(), jnp.zeros((16, 96), f32)], axis=1)
    rows = lax.broadcasted_iota(jnp.int32, (16, 128), 0)
    pivots = jnp.zeros((16, 128), f32)
    for j in range(16):
        column = jnp.broadcast_to(work[:, j : j + 1], (16, 128))
        pivot = jnp.broadcast_to(column[j : j + 1], (16, 128))
        row = jnp.broadcast_to(work[j : j + 1], (16, 128))
        pivots = jnp.where(rows == j, pivot, pivots)
        work = work - jnp.where(rows > j, column / pivot, 0.0) * row
    scaled = work / jnp.sqrt(pivots)
    upper = jnp.where(
        lax.broadcasted_iota(jnp.int32, (16, 16), 0) <= lax.broadcasted_iota(jnp.int32, (16, 16), 1),
        scaled[:, 0:16],
        0.0,
    )
    return upper, scaled[:, 16:32]


def update_kernel(step, node_total, *refs):
    refs = list(refs)
    take = lambda count: [refs.pop(0) for _ in range(count)]
    (arrived,) = take(1)
    own, one, two, three = take(4)
    before, degree = (None, None) if step == 0 else take(2)
    shift_in = take(1)[0] if step > 1 else None
    (start,) = take(1) if step == 0 else (None,)
    outs = refs
    side = own[...] + one[...] + two[...] + three[...]
    height = arrived.shape[1]
    total = side[0:height]
    for p in range(arrived.shape[0]):
        total = total + arrived[p]
    gram = unpack_gram(side[height : height + 8]) * (1.0 / node_total)
    if step == 0:
        packed, state, degree_out, upper_out = outs
        level = total[16:17]
        upper, inverse = factor_and_inverse(gram[:, 0:16])
        block = start[...]
        applied = level * block - total[0:16]
        both = dot_f32(inverse, jnp.concatenate([block, applied], axis=1), ((1,), (0,)))
        degree_out[...] = total[16:24]
        stack = both
        new_vectors = both[:, 0:256]
        new_applied = both[:, 256:512]
        state[...] = both
        basis = new_vectors
        upper_out[...] = upper
    else:
        if step == 1:
            packed, state, coeff_out, upper_out, shift_out = outs
        else:
            packed, state, coeff_out, upper_out = outs
        width = 16 * step
        coeffs = gram[:, 0:width]
        square = gram[:, width : width + 16]
        square = square - dot_f32(coeffs, coeffs, ((1,), (1,)))
        upper, inverse = factor_and_inverse(square)
        stack = before[...]
        newest = stack[width - 16 : width]
        vectors, applied = newest[:, 0:256], newest[:, 256:512]
        level = degree[0:1]
        twice = level * applied - total[0:16]
        coeff_out[...] = jnp.concatenate([coeffs, jnp.zeros((16, 128 - width), f32)], axis=1)
        if step == 1:
            shift = jnp.broadcast_to(
                jnp.sum(coeffs * eye16(), axis=(0, 1), keepdims=True) * (1.0 / 16), (8, 128)
            )
            shift_out[...] = shift
            scalar = shift[0:1, 0:1]
            moved = applied - scalar * vectors
            twice = twice - scalar * applied - scalar * moved
            coeffs = coeffs - scalar * eye16()
            applied = moved
            stack = jnp.concatenate([vectors, applied], axis=1)
        else:
            scalar = shift_in[0:1, 0:1]
            twice = twice - scalar * applied
            coeff_out[:, width - 16 : width] = coeffs[:, width - 16 : width] + scalar * eye16()
        rest = jnp.concatenate([applied, twice], axis=1) - dot_f32(coeffs, stack, ((1,), (0,)))
        both = dot_f32(inverse, rest, ((1,), (0,)))
        state[0:width] = stack
        state[width : width + 16] = both
        upper_out[...] = upper
        new_applied = both[:, 256:512]
        basis = jnp.concatenate([stack[:, 0:256], both[:, 0:256]], axis=0)
    partial = dot_f32(new_applied, jnp.concatenate([basis, new_applied], axis=0), ((1,), (1,)))
    message = jnp.concatenate([new_applied, pack_gram(partial)], axis=0)
    for p in range(packed.shape[0]):
        packed[p] = message


def update(step, node_total, arrived, sides, state, degree, shift, start):
    size = arrived.shape[2]
    shapes = [
        jax.ShapeDtypeStruct((16, 24, size), f32),
        jax.ShapeDtypeStruct((16 * (step + 1), 2 * size), f32),
    ]
    if step == 0:
        shapes += [jax.ShapeDtypeStruct((8, size), f32), jax.ShapeDtypeStruct((16, 16), f32)]
        extra = [start]
    else:
        shapes += [jax.ShapeDtypeStruct((16, 128), f32), jax.ShapeDtypeStruct((16, 16), f32)]
        extra = [state, degree]
        if step == 1:
            shapes.append(jax.ShapeDtypeStruct((8, 128), f32))
        else:
            extra.append(shift)
    args = [arrived, *sides, *extra]
    return pl.pallas_call(
        functools.partial(update_kernel, step, node_total),
        name=f"update_{step}",
        out_shape=tuple(shapes),
        in_specs=[VMEM] * len(args),
        out_specs=(VMEM,) * len(shapes),
        cost_estimate=pl.CostEstimate(flops=400_000_000, bytes_accessed=1 << 20, transcendentals=0),
    )(*args)


def last_kernel(node_total, arrived, state, shift, block_out, coeff_out, upper_out):
    packed = arrived[0]
    for p in range(1, arrived.shape[0]):
        packed = packed + arrived[p]
    gram = unpack_gram(packed) * (1.0 / node_total)
    width = 16 * ITERS
    coeffs = gram[:, 0:width]
    square = gram[:, width : width + 16] - dot_f32(coeffs, coeffs, ((1,), (1,)))
    upper, inverse = factor_and_inverse(square)
    stack = state[...]
    rest = stack[width - 16 : width, 256:512] - dot_f32(coeffs, stack[:, 0:256], ((1,), (0,)))
    block_out[...] = dot_f32(inverse, rest, ((1,), (0,)))
    coeff_out[...] = jnp.concatenate([coeffs, jnp.zeros((16, 128 - width), f32)], axis=1)
    coeff_out[:, width - 16 : width] = coeffs[:, width - 16 : width] + shift[0:1, 0:1] * eye16()
    upper_out[...] = upper


def last(node_total, arrived, state, shift):
    size = 256
    return pl.pallas_call(
        functools.partial(last_kernel, node_total),
        name="last",
        out_shape=(
            jax.ShapeDtypeStruct((16, size), f32),
            jax.ShapeDtypeStruct((16, 128), f32),
            jax.ShapeDtypeStruct((16, 16), f32),
        ),
        in_specs=[VMEM] * 3,
        out_specs=(VMEM,) * 3,
    )(arrived, state, shift)


def first_message_kernel(block, packed):
    partial = dot_f32(block[...], block[...], ((1,), (1,)))
    message = jnp.concatenate([block[...], pack_gram(partial)], axis=0)
    for p in range(packed.shape[0]):
        packed[p] = message


def first_message(block):
    return pl.pallas_call(
        first_message_kernel,
        name="first_message",
        out_shape=jax.ShapeDtypeStruct((16, 24, block.shape[1]), f32),
        in_specs=[VMEM],
        out_specs=VMEM,
    )(block)


def shifted(value, hop):
    size = lax.axis_size("grp")
    return lax.ppermute(value, "grp", [(i, (i + hop) % size) for i in range(size)])


def swapped(value):
    return lax.ppermute(value, CORE, [(0, 1), (1, 0)])


def exchanged(value, axes):
    return lax.all_to_all(value, axes, split_axis=0, concat_axis=0, tiled=True)


def body(start_block, tile_values, tile_row, tile_col, tile_count):
    grp_size = lax.axis_size("grp")
    col_size = lax.axis_size(ZX) * lax.axis_size(CORE)
    node_total = float(start_block.shape[1] * grp_size * col_size)
    grp_index = lax.axis_index("grp")
    core_index = lax.axis_index(CORE)
    local_row = tile_row[0, 0] - grp_index * col_size
    home = tile_col[0, 0] // col_size
    info = jnp.stack(
        [
            local_row // 2,
            (local_row % 2) ^ core_index,
            (grp_index - home + grp_size) % grp_size,
            (home - grp_index + grp_size) % grp_size,
            jnp.broadcast_to(tile_count[0, 0], local_row.shape),
        ]
    )
    info = jnp.where(
        jnp.array([[15], [1], [3], [3], [1 << 20]], jnp.int32) < info, 0, jnp.maximum(info, 0)
    )
    message = first_message(start_block)
    piece = start_block
    state = degree = shift = None
    uppers, coeffs = [], []
    for step in range(ITERS):
        first = step == 0
        near = exchanged(message, ZX)
        pieces = [piece] + [shifted(piece, hop) for hop in range(1, grp_size)]
        mine, other = rows_product(first, info, tile_values, pieces)
        far = swapped(near)
        rows = mine + swapped(other)
        arrived = exchanged(rows, ZX)
        sides = cols_product(first, info, tile_values, near, far)
        sides = [sides[0]] + [shifted(sides[hop], hop) for hop in range(1, grp_size)]
        outs = update(step, node_total, arrived, sides, state, degree, shift, start_block)
        message, state = outs[0], outs[1]
        piece = message[0, 0:16]
        if first:
            degree = outs[2]
        else:
            coeffs.append(outs[2])
        uppers.append(outs[3])
        if step == 1:
            shift = outs[4]
    packed = message[0, 16:24].reshape(1, -1)
    packed = exchanged(jnp.broadcast_to(packed, (16, *packed.shape)), ("grp", "col_1")).sum(0)
    packed = exchanged(jnp.broadcast_to(packed, (8, *packed.shape)), ("col_0", "col_2"))
    block, coeff, upper = last(node_total, packed.reshape(8, 8, 256), state, shift)
    coeffs.append(coeff)
    uppers.append(upper)
    basis = jnp.concatenate(
        [state[:, 0:256].reshape(ITERS, 16, 256), block[None]], axis=0
    )
    shaped = jnp.stack(coeffs)[:, :, 0 : 16 * ITERS].reshape(ITERS, 16, ITERS, 16)
    return basis, shaped.transpose(0, 2, 1, 3), jnp.stack(uppers).transpose(0, 2, 1)


def solution(mesh):
    split_mesh = Mesh(
        mesh.devices.reshape(mesh.shape["grp"], 4, 4, 2), ("grp", "col_0", "col_1", "col_2")
    )
    col = ("col_0", "col_1", "col_2")
    placed = (
        P(None, GRP_COL),
        P("grp", col, None, None, None),
        P("grp", col, None),
        P("grp", col, None),
        P("grp", col),
    )
    return jax.shard_map(
        body,
        mesh=split_mesh,
        in_specs=placed,
        out_specs=(P(None, None, GRP_COL), P(), P()),
        check_vma=False,
    )
```

```python
import functools
import jax
import jax.numpy as jnp
from jax import lax
from jax.experimental import pallas as pl
from jax.experimental.pallas import tpu as pltpu
from jax.sharding import Mesh
from jax.sharding import PartitionSpec as P

ITERS = 4
ZX = ("col_0", "col_1")
CORE = "col_2"
COL = ("col_0", "col_1", "col_2")
GRP_COL = ("grp", "col_0", "col_1", "col_2")
GROUP = 8
highest = lax.Precision.HIGHEST
VMEM = pl.BlockSpec(memory_space=pltpu.VMEM)
SMEM = pl.BlockSpec(memory_space=pltpu.SMEM)
HBM = pl.BlockSpec(memory_space=pltpu.MemorySpace.HBM)
MIB = 1 << 20
f32 = jnp.float32
bf16 = jnp.bfloat16


def split(x):
    hi = x.astype(bf16)
    return hi, (x - hi.astype(f32)).astype(bf16)


def dot(a, b, dims):
    return lax.dot_general(a, b, (dims, ((), ())), preferred_element_type=f32)


def dot_f32(a, b, dims):
    return lax.dot_general(a, b, (dims, ((), ())), precision=highest, preferred_element_type=f32)


def limits(mib):
    return pltpu.CompilerParams(vmem_limit_bytes=mib * MIB)


def cost(flops):
    return pl.CostEstimate(flops=flops, bytes_accessed=MIB, transcendentals=0)


def products(lhs_hi, lhs_lo, hi, lo, dims, first, live):
    top = dot(lhs_hi, hi, dims)
    low = dot(lhs_lo, lo, dims)
    out = top[0:16] + top[16:32] + low[0:16]
    if first:
        out = jnp.concatenate([out, top[32:40] + low[16:24]], axis=0)
    return out * live


def stacked_lhs(piece, first):
    hi, lo = split(piece)
    if first:
        ones = jnp.ones((16, piece.shape[1]), bf16)
        return jnp.concatenate([hi, lo, ones], axis=0), jnp.concatenate([hi, ones], axis=0)
    return jnp.concatenate([hi, lo], axis=0), hi


def fill_pieces(pieces, lhs_hi, lhs_lo, first):
    for k, piece in enumerate(pieces):
        lhs_hi[k], lhs_lo[k] = stacked_lhs(piece[...], first)


def group_rows(base, place, lhs_hi, lhs_lo, hi, lo, out, first):
    tile_row, tile_col, tile_count = place
    results = []
    for u in range(GROUP):
        s = base + u
        k = ((tile_row[0, 0, 0] >> 5) - (tile_col[0, 0, s] >> 5)) & 3
        live = (s < tile_count[0, 0]).astype(f32)
        results.append(
            products(lhs_hi[k], lhs_lo[k], hi[s], lo[s], ((1,), (1,)), first, live)
        )
    for u in range(GROUP):
        out[tile_row[0, 0, base + u] & 31] += results[u]


def rows_first_kernel(
    tile_row, tile_col, tile_count, tiles, own, one, two, three, out, hi, lo, buf, lhs_hi, lhs_lo, sems
):
    slots = buf.shape[0]
    copies = [
        pltpu.make_async_copy(
            tiles.at[0, 0, pl.ds(q * GROUP, GROUP)], buf.at[pl.ds(q * GROUP, GROUP)], sems.at[q]
        )
        for q in range(slots // GROUP)
    ]
    for copy in copies:
        copy.start()
    fill_pieces((own, one, two, three), lhs_hi, lhs_lo, True)
    out[...] = jnp.zeros_like(out)
    for q, copy in enumerate(copies):
        copy.wait()
        for u in range(GROUP):
            s = q * GROUP + u
            hi[s], lo[s] = split(buf[s])

        @pl.when(q * GROUP < tile_count[0, 0])
        def _():
            group_rows(
                q * GROUP, (tile_row, tile_col, tile_count), lhs_hi, lhs_lo, hi, lo, out, True
            )


def groups_of(tile_count):
    return (tile_count[0, 0] + (GROUP - 1)) // GROUP


def rows_next_kernel(
    tile_row, tile_col, tile_count, hi, lo, own, one, two, three, out, lhs_hi, lhs_lo
):
    fill_pieces((own, one, two, three), lhs_hi, lhs_lo, False)
    out[...] = jnp.zeros_like(out)

    @pl.loop(0, groups_of(tile_count))
    def _(q):
        group_rows(q * GROUP, (tile_row, tile_col, tile_count), lhs_hi, lhs_lo, hi, lo, out, False)


def cols_kernel(
    first, tile_row, tile_col, tile_count, hi, lo, near, far, own, one, two, three, acc
):
    acc[...] = jnp.zeros_like(acc)
    gram = jnp.zeros_like(near[0, 16:24])
    for p in range(near.shape[0]):
        gram = gram + (near[p, 16:24] + far[p, 16:24])

    @pl.loop(0, groups_of(tile_count))
    def _(q):
        results, slots = [], []
        for u in range(GROUP):
            s = q * GROUP + u
            row = tile_row[0, 0, s] & 31
            place = row >> 1
            same = ((row ^ tile_col[0, 0, 0]) & 1) == 0
            piece = jnp.where(same, near[place, 0:16], far[place, 0:16])
            left_hi, left_lo = stacked_lhs(piece, first)
            live = (s < tile_count[0, 0]).astype(f32)
            results.append(
                products(left_hi, left_lo, hi[s], lo[s], ((1,), (0,)), first, live)
            )
            slots.append(((tile_col[0, 0, s] >> 5) - (tile_row[0, 0, 0] >> 5)) & 3)
        for u in range(GROUP):
            acc[slots[u]] += results[u]

    for k, out in enumerate((own, one, two, three)):
        out[...] = jnp.concatenate([acc[k], gram], axis=0)


def rows_first(place, tiles, pieces):
    slots, size = tiles.shape[2], tiles.shape[3]
    return pl.pallas_call(
        rows_first_kernel,
        name="rows_first",
        out_shape=(
            jax.ShapeDtypeStruct((32, 24, size), f32),
            pltpu.VMEM((slots, size, size), bf16),
            pltpu.VMEM((slots, size, size), bf16),
        ),
        in_specs=[SMEM] * 3 + [HBM] + [VMEM] * 4,
        out_specs=(VMEM,) * 3,
        scratch_shapes=[
            pltpu.VMEM((slots, size, size), f32),
            pltpu.VMEM((4, 48, size), bf16),
            pltpu.VMEM((4, 32, size), bf16),
            pltpu.SemaphoreType.DMA((slots // GROUP,)),
        ],
        compiler_params=limits(28),
        cost_estimate=cost(400_000_000),
    )(*place, tiles, *pieces)


def rows_next(place, hi, lo, pieces):
    size = hi.shape[1]
    return pl.pallas_call(
        rows_next_kernel,
        name="rows_next",
        out_shape=jax.ShapeDtypeStruct((32, 16, size), f32),
        in_specs=[SMEM] * 3 + [VMEM] * 6,
        out_specs=VMEM,
        scratch_shapes=[pltpu.VMEM((4, 32, size), bf16), pltpu.VMEM((4, 16, size), bf16)],
        compiler_params=limits(20),
        cost_estimate=cost(400_000_000),
    )(*place, hi, lo, *pieces)


def cols_product(first, place, hi, lo, near, far):
    height = 24 if first else 16
    size = hi.shape[1]
    out = jax.ShapeDtypeStruct((height + 8, size), f32)
    return pl.pallas_call(
        functools.partial(cols_kernel, first),
        name="cols_first" if first else "cols_next",
        out_shape=(out,) * 4,
        in_specs=[SMEM] * 3 + [VMEM] * 4,
        out_specs=(VMEM,) * 4,
        scratch_shapes=[pltpu.VMEM((4, height, size), f32)],
        compiler_params=limits(20),
        cost_estimate=cost(400_000_000),
    )(*place, hi, lo, near, far)


def unpack_gram(packed):
    return jnp.concatenate([packed[:, 0:128], packed[:, 128:256]], axis=0)


def pack_gram(gram):
    width = gram.shape[1]
    if width < 128:
        gram = jnp.concatenate([gram, jnp.zeros((16, 128 - width), f32)], axis=1)
    return jnp.concatenate([gram[0:8], gram[8:16]], axis=1)


def eye16():
    return (
        lax.broadcasted_iota(jnp.int32, (16, 16), 0) == lax.broadcasted_iota(jnp.int32, (16, 16), 1)
    ).astype(f32)


def factor_and_inverse(gram):
    work = jnp.concatenate([gram, eye16(), jnp.zeros((16, 96), f32)], axis=1)
    rows = lax.broadcasted_iota(jnp.int32, (16, 128), 0)
    lanes = lax.broadcasted_iota(jnp.int32, (16, 128), 1)
    down = jnp.ones((16, 128), f32)
    across = jnp.ones((16, 128), f32)
    lower = jnp.zeros((16, 128), f32)
    for j in range(16):
        column = jnp.broadcast_to(work[:, j : j + 1], (16, 128))
        pivot = jnp.broadcast_to(column[j : j + 1], (16, 128))
        row = jnp.broadcast_to(work[j : j + 1], (16, 128))
        down = jnp.where(rows == j, pivot, down)
        across = jnp.where(lanes == j, pivot, across)
        lower = jnp.where((lanes == j) & (rows >= j), column, lower)
        work = work - jnp.where(rows > j, column / pivot, 0.0) * row
    lower = lower / jnp.sqrt(across)
    inverse = work / jnp.sqrt(down)
    return lower[:, 0:16], inverse[:, 16:32]


def update_kernel(step, node_total, *refs):
    refs = list(refs)
    take = lambda count: [refs.pop(0) for _ in range(count)]
    (arrived,) = take(1)
    own, one, two, three = take(4)
    before, degree = (None, None) if step == 0 else take(2)
    shift_in = take(1)[0] if step > 1 else None
    (start,) = take(1) if step == 0 else (None,)
    outs = refs
    side = own[...] + one[...] + two[...] + three[...]
    height = arrived.shape[1]
    total = side[0:height]
    for p in range(arrived.shape[0]):
        total = total + arrived[p]
    gram = unpack_gram(side[height : height + 8]) * (1.0 / node_total)
    if step == 0:
        packed, piece_out, state, degree_out, lower_out = outs
        level = total[16:17]
        lower, inverse = factor_and_inverse(gram[:, 0:16])
        block = start[...]
        applied = level * block - total[0:16]
        both = dot_f32(inverse, jnp.concatenate([block, applied], axis=1), ((1,), (0,)))
        degree_out[...] = total[16:24]
        stack = both
        new_vectors = both[:, 0:256]
        new_applied = both[:, 256:512]
        state[...] = both
        basis = new_vectors
        lower_out[...] = lower
    else:
        if step == 1:
            packed, piece_out, state, coeff_out, lower_out, shift_out = outs
        else:
            packed, piece_out, state, coeff_out, lower_out = outs
        width = 16 * step
        coeffs = gram[:, 0:width]
        square = gram[:, width : width + 16]
        square = square - dot_f32(coeffs, coeffs, ((1,), (1,)))
        lower, inverse = factor_and_inverse(square)
        stack = before[...]
        newest = stack[width - 16 : width]
        vectors, applied = newest[:, 0:256], newest[:, 256:512]
        level = degree[0:1]
        twice = level * applied - total[0:16]
        coeff_out[...] = jnp.concatenate([coeffs, jnp.zeros((16, 128 - width), f32)], axis=1)
        if step == 1:
            shift = jnp.broadcast_to(
                jnp.sum(coeffs * eye16(), axis=(0, 1), keepdims=True) * (1.0 / 16), (8, 128)
            )
            shift_out[...] = shift
            scalar = shift[0:1, 0:1]
            moved = applied - scalar * vectors
            twice = twice - scalar * applied - scalar * moved
            coeffs = coeffs - scalar * eye16()
            applied = moved
            stack = jnp.concatenate([vectors, applied], axis=1)
        else:
            scalar = shift_in[0:1, 0:1]
            twice = twice - scalar * applied
            coeff_out[:, width - 16 : width] = coeffs[:, width - 16 : width] + scalar * eye16()
        rest = jnp.concatenate([applied, twice], axis=1) - dot_f32(coeffs, stack, ((1,), (0,)))
        both = dot_f32(inverse, rest, ((1,), (0,)))
        state[0:width] = stack
        state[width : width + 16] = both
        lower_out[...] = lower
        new_applied = both[:, 256:512]
        basis = jnp.concatenate([stack[:, 0:256], both[:, 0:256]], axis=0)
    partial = dot_f32(new_applied, jnp.concatenate([basis, new_applied], axis=0), ((1,), (1,)))
    piece_out[...] = new_applied
    gram_rows = pack_gram(partial)
    if step == ITERS - 1:
        for p in range(packed.shape[0]):
            packed[p] = gram_rows
    else:
        message = jnp.concatenate([new_applied, gram_rows], axis=0)
        for p in range(packed.shape[0]):
            packed[p] = message


def update(step, node_total, arrived, sides, state, degree, shift, start):
    size = arrived.shape[2]
    shapes = [
        jax.ShapeDtypeStruct((8, 8, size) if step == ITERS - 1 else (16, 24, size), f32),
        jax.ShapeDtypeStruct((16, size), f32),
        jax.ShapeDtypeStruct((16 * (step + 1), 2 * size), f32),
    ]
    if step == 0:
        shapes += [jax.ShapeDtypeStruct((8, size), f32), jax.ShapeDtypeStruct((16, 16), f32)]
        extra = [start]
    else:
        shapes += [jax.ShapeDtypeStruct((16, 128), f32), jax.ShapeDtypeStruct((16, 16), f32)]
        extra = [state, degree]
        if step == 1:
            shapes.append(jax.ShapeDtypeStruct((8, 128), f32))
        else:
            extra.append(shift)
    args = [arrived, *sides, *extra]
    return pl.pallas_call(
        functools.partial(update_kernel, step, node_total),
        name=f"update_{step}",
        out_shape=tuple(shapes),
        in_specs=[VMEM] * len(args),
        out_specs=(VMEM,) * len(shapes),
        compiler_params=limits(16),
        cost_estimate=cost(400_000_000),
    )(*args)


def fold_kernel(arrived, packed):
    total = arrived[0]
    for p in range(1, arrived.shape[0]):
        total = total + arrived[p]
    for p in range(packed.shape[0]):
        packed[p] = total


def fold(arrived):
    return pl.pallas_call(
        fold_kernel,
        name="fold",
        out_shape=jax.ShapeDtypeStruct((16, 8, arrived.shape[2]), f32),
        in_specs=[VMEM],
        out_specs=VMEM,
        compiler_params=limits(8),
    )(arrived)


def last_kernel(node_total, arrived, state, shift, *refs):
    coeffs_in, lowers_in = refs[0 : ITERS - 1], refs[ITERS - 1 : 2 * ITERS - 1]
    basis_out, coeffs_out, lowers_out = refs[2 * ITERS - 1 :]
    packed = arrived[0]
    for p in range(1, arrived.shape[0]):
        packed = packed + arrived[p]
    gram = unpack_gram(packed) * (1.0 / node_total)
    width = 16 * ITERS
    coeffs = gram[:, 0:width]
    square = gram[:, width : width + 16] - dot_f32(coeffs, coeffs, ((1,), (1,)))
    stack = state[...]
    rest = stack[width - 16 : width, 256:512] - dot_f32(coeffs, stack[:, 0:256], ((1,), (0,)))
    for k in range(ITERS):
        basis_out[k] = stack[16 * k : 16 * k + 16, 0:256]
        lowers_out[k] = lowers_in[k][...]
        for j in range(ITERS):
            if j > k:
                coeffs_out[k, j] = jnp.zeros((16, 16), f32)
            elif k < ITERS - 1:
                coeffs_out[k, j] = coeffs_in[k][:, 16 * j : 16 * j + 16]
            elif j < k:
                coeffs_out[k, j] = coeffs[:, 16 * j : 16 * j + 16]
            else:
                coeffs_out[k, j] = coeffs[:, 16 * j : 16 * j + 16] + shift[0:1, 0:1] * eye16()
    lower, inverse = factor_and_inverse(square)
    basis_out[ITERS] = dot_f32(inverse, rest, ((1,), (0,)))
    lowers_out[ITERS] = lower


def last(node_total, arrived, state, shift, coeffs, lowers):
    args = [arrived, state, shift, *coeffs, *lowers]
    return pl.pallas_call(
        functools.partial(last_kernel, node_total),
        name="last",
        out_shape=(
            jax.ShapeDtypeStruct((ITERS + 1, 16, arrived.shape[2]), f32),
            jax.ShapeDtypeStruct((ITERS, ITERS, 16, 16), f32),
            jax.ShapeDtypeStruct((ITERS + 1, 16, 16), f32),
        ),
        in_specs=[VMEM] * len(args),
        out_specs=(VMEM,) * 3,
        compiler_params=limits(8),
    )(*args)


def first_message_kernel(block, packed):
    partial = dot_f32(block[...], block[...], ((1,), (1,)))
    message = jnp.concatenate([block[...], pack_gram(partial)], axis=0)
    for p in range(packed.shape[0]):
        packed[p] = message


def first_message(block):
    return pl.pallas_call(
        first_message_kernel,
        name="first_message",
        out_shape=jax.ShapeDtypeStruct((16, 24, block.shape[1]), f32),
        in_specs=[VMEM],
        out_specs=VMEM,
        compiler_params=limits(8),
    )(block)


def shifted(value, hop):
    size = lax.axis_size("grp")
    return lax.ppermute(value, "grp", [(i, (i + hop) % size) for i in range(size)])


def swapped(value):
    return lax.ppermute(value, CORE, [(0, 1), (1, 0)])


def exchanged(value, axes):
    return lax.all_to_all(value, axes, split_axis=0, concat_axis=0, tiled=True)


def body(start_block, tile_values, tile_row, tile_col, tile_count):
    grp_size = lax.axis_size("grp")
    node_total = float(start_block.shape[1] * grp_size * lax.axis_size(COL))
    place = (tile_row, tile_col, tile_count)
    message = first_message(start_block)
    piece = start_block
    state = degree = shift = hi = lo = None
    lowers, coeffs = [], []
    for step in range(ITERS):
        first = step == 0
        pieces = [piece] + [shifted(piece, hop) for hop in range(1, grp_size)]
        near = exchanged(message, ZX)
        if first:
            rows, hi, lo = rows_first(place, tile_values, pieces)
        else:
            rows = rows_next(place, hi, lo, pieces)
        far = swapped(near)
        arrived = exchanged(rows, COL)
        sides = cols_product(first, place, hi, lo, near, far)
        sides = [sides[0]] + [shifted(sides[hop], hop) for hop in range(1, grp_size)]
        outs = update(step, node_total, arrived, sides, state, degree, shift, start_block)
        message, piece, state = outs[0:3]
        if first:
            degree = outs[3]
        else:
            coeffs.append(outs[3])
        lowers.append(outs[4])
        if step == 1:
            shift = outs[5]
    packed = fold(exchanged(message, ("col_1", "col_2")))
    packed = exchanged(packed, ("grp", "col_0"))
    return last(node_total, packed, state, shift, coeffs, lowers)


def solution(mesh):
    split_mesh = Mesh(
        mesh.devices.reshape(mesh.shape["grp"], 4, 4, 2), ("grp", "col_0", "col_1", "col_2")
    )
    placed = (
        P(None, GRP_COL),
        P("grp", COL, None, None, None),
        P("grp", COL, None),
        P("grp", COL, None),
        P("grp", COL),
    )
    return jax.shard_map(
        body,
        mesh=split_mesh,
        in_specs=placed,
        out_specs=(P(None, None, GRP_COL), P(), P()),
        check_vma=False,
    )
```

```python
import functools
import jax
import jax.numpy as jnp
from jax import lax
from jax.experimental import pallas as pl
from jax.experimental.pallas import tpu as pltpu
from jax.sharding import Mesh
from jax.sharding import PartitionSpec as P

ITERS = 4
ZX = ("col_0", "col_1")
CORE = "col_2"
COL = ("col_0", "col_1", "col_2")
GRP_COL = ("grp", "col_0", "col_1", "col_2")
ROW_GROUP = 8
COL_GROUP = 4
highest = lax.Precision.HIGHEST
VMEM = pl.BlockSpec(memory_space=pltpu.VMEM)
SMEM = pl.BlockSpec(memory_space=pltpu.SMEM)
HBM = pl.BlockSpec(memory_space=pltpu.MemorySpace.HBM)
MIB = 1 << 20
f32 = jnp.float32
bf16 = jnp.bfloat16


def split(x):
    hi = x.astype(bf16)
    return hi, (x - hi.astype(f32)).astype(bf16)


def dot(a, b, dims):
    return lax.dot_general(a, b, (dims, ((), ())), preferred_element_type=f32)


def dot_f32(a, b, dims):
    return lax.dot_general(a, b, (dims, ((), ())), precision=highest, preferred_element_type=f32)


def limits(mib):
    return pltpu.CompilerParams(vmem_limit_bytes=mib * MIB)


def cost(flops):
    return pl.CostEstimate(flops=flops, bytes_accessed=MIB, transcendentals=0)


def products(lhs_hi, lhs_lo, hi, lo, dims, first, live):
    top = dot(lhs_hi, hi, dims)
    low = dot(lhs_lo, lo, dims)
    out = top[0:16] + top[16:32] + low[0:16]
    if first:
        out = jnp.concatenate([out, top[32:40] + low[16:24]], axis=0)
    return out * live


def stacked_lhs(piece, first):
    hi, lo = split(piece)
    if first:
        ones = jnp.ones((16, piece.shape[1]), bf16)
        return jnp.concatenate([hi, lo, ones], axis=0), jnp.concatenate([hi, ones], axis=0)
    return jnp.concatenate([hi, lo], axis=0), hi


def fill_pieces(pieces, lhs_hi, lhs_lo, first):
    for k, piece in enumerate(pieces):
        lhs_hi[k], lhs_lo[k] = stacked_lhs(piece[...], first)


def group_rows(base, place, lhs_hi, lhs_lo, hi, lo, out, first):
    tile_row, tile_col, tile_count = place
    results = []
    for u in range(ROW_GROUP):
        s = base + u
        k = ((tile_row[0, 0, 0] >> 5) - (tile_col[0, 0, s] >> 5)) & 3
        live = (s < tile_count[0, 0]).astype(f32)
        results.append(
            products(lhs_hi[k], lhs_lo[k], hi[s], lo[s], ((1,), (1,)), first, live)
        )
    for u in range(ROW_GROUP):
        out[tile_row[0, 0, base + u] & 31] += results[u]


def groups_of(tile_count, group):
    return (tile_count[0, 0] + (group - 1)) // group


def group_copies(q, group, source_hi, source_lo, hi, lo, sems):
    part = pl.ds(q * group, group)
    return (
        pltpu.make_async_copy(source_hi.at[part], hi.at[part], sems.at[0, q]),
        pltpu.make_async_copy(source_lo.at[part], lo.at[part], sems.at[1, q]),
    )


def start_groups(tile_count, group, *refs):
    @pl.loop(0, groups_of(tile_count, group))
    def _(q):
        for copy in group_copies(q, group, *refs):
            copy.start()


def rows_first_kernel(
    tile_row, tile_col, tile_count, tiles, own, one, two, three, out, hi_out, lo_out,
    buf, hi, lo, lhs_hi, lhs_lo, sems, out_sems
):
    group = ROW_GROUP
    count = groups_of(tile_count, group)

    def arriving(q):
        part = pl.ds(q * group, group)
        return pltpu.make_async_copy(tiles.at[0, 0, part], buf.at[part], sems.at[q])

    @pl.loop(0, count)
    def _(q):
        arriving(q).start()

    fill_pieces((own, one, two, three), lhs_hi, lhs_lo, True)
    out[...] = jnp.zeros_like(out)

    @pl.loop(0, count)
    def _(q):
        arriving(q).wait()
        for u in range(group):
            s = q * group + u
            hi[s], lo[s] = split(buf[s])
        for copy in group_copies(q, group, hi, lo, hi_out, lo_out, out_sems):
            copy.start()
        group_rows(
            q * group, (tile_row, tile_col, tile_count), lhs_hi, lhs_lo, hi, lo, out, True
        )

    @pl.loop(0, count)
    def _(q):
        for copy in group_copies(q, group, hi, lo, hi_out, lo_out, out_sems):
            copy.wait()


def rows_next_kernel(
    tile_row, tile_col, tile_count, hi_in, lo_in, own, one, two, three, out, hi, lo, lhs_hi, lhs_lo, sems
):
    group = ROW_GROUP
    start_groups(tile_count, group, hi_in, lo_in, hi, lo, sems)
    fill_pieces((own, one, two, three), lhs_hi, lhs_lo, False)
    out[...] = jnp.zeros_like(out)

    @pl.loop(0, groups_of(tile_count, group))
    def _(q):
        for copy in group_copies(q, group, hi_in, lo_in, hi, lo, sems):
            copy.wait()
        group_rows(q * group, (tile_row, tile_col, tile_count), lhs_hi, lhs_lo, hi, lo, out, False)


def cols_kernel(
    first, tile_row, tile_col, tile_count, hi_in, lo_in, near, far, own, one, two, three,
    hi, lo, acc, sems
):
    group = COL_GROUP
    start_groups(tile_count, group, hi_in, lo_in, hi, lo, sems)
    acc[...] = jnp.zeros_like(acc)
    gram = jnp.zeros_like(near[0, 16:24])
    for p in range(near.shape[0]):
        gram = gram + (near[p, 16:24] + far[p, 16:24])

    @pl.loop(0, groups_of(tile_count, group))
    def _(q):
        for copy in group_copies(q, group, hi_in, lo_in, hi, lo, sems):
            copy.wait()
        results, slots = [], []
        for u in range(group):
            s = q * group + u
            row = tile_row[0, 0, s] & 31
            place = row >> 1
            same = ((row ^ tile_col[0, 0, 0]) & 1) == 0
            piece = jnp.where(same, near[place, 0:16], far[place, 0:16])
            left_hi, left_lo = stacked_lhs(piece, first)
            live = (s < tile_count[0, 0]).astype(f32)
            results.append(
                products(left_hi, left_lo, hi[s], lo[s], ((1,), (0,)), first, live)
            )
            slots.append(((tile_col[0, 0, s] >> 5) - (tile_row[0, 0, 0] >> 5)) & 3)
        for u in range(group):
            acc[slots[u]] += results[u]

    for k, out in enumerate((own, one, two, three)):
        out[...] = jnp.concatenate([acc[k], gram], axis=0)


def rows_first(place, tiles, pieces):
    slots, size = tiles.shape[2], tiles.shape[3]
    return pl.pallas_call(
        rows_first_kernel,
        name="rows_first",
        out_shape=(
            jax.ShapeDtypeStruct((32, 24, size), f32),
            pltpu.MemorySpace.HBM((slots, size, size), bf16),
            pltpu.MemorySpace.HBM((slots, size, size), bf16),
        ),
        in_specs=[SMEM] * 3 + [HBM] + [VMEM] * 4,
        out_specs=(VMEM, HBM, HBM),
        scratch_shapes=[
            pltpu.VMEM((slots, size, size), f32),
            pltpu.VMEM((slots, size, size), bf16),
            pltpu.VMEM((slots, size, size), bf16),
            pltpu.VMEM((4, 48, size), bf16),
            pltpu.VMEM((4, 32, size), bf16),
            pltpu.SemaphoreType.DMA((slots // ROW_GROUP,)),
            pltpu.SemaphoreType.DMA((2, slots // ROW_GROUP)),
        ],
        compiler_params=limits(28),
        cost_estimate=cost(400_000_000),
    )(*place, tiles, *pieces)


def rows_next(place, hi, lo, pieces):
    slots, size = hi.shape[0], hi.shape[1]
    return pl.pallas_call(
        rows_next_kernel,
        name="rows_next",
        out_shape=jax.ShapeDtypeStruct((32, 16, size), f32),
        in_specs=[SMEM] * 3 + [HBM] * 2 + [VMEM] * 4,
        out_specs=VMEM,
        scratch_shapes=[
            pltpu.VMEM((slots, size, size), bf16),
            pltpu.VMEM((slots, size, size), bf16),
            pltpu.VMEM((4, 32, size), bf16),
            pltpu.VMEM((4, 16, size), bf16),
            pltpu.SemaphoreType.DMA((2, slots // ROW_GROUP)),
        ],
        compiler_params=limits(20),
        cost_estimate=cost(400_000_000),
    )(*place, hi, lo, *pieces)


def cols_product(first, place, hi, lo, near, far):
    height = 24 if first else 16
    slots, size = hi.shape[0], hi.shape[1]
    out = jax.ShapeDtypeStruct((height + 8, size), f32)
    return pl.pallas_call(
        functools.partial(cols_kernel, first),
        name="cols_first" if first else "cols_next",
        out_shape=(out,) * 4,
        in_specs=[SMEM] * 3 + [HBM] * 2 + [VMEM] * 2,
        out_specs=(VMEM,) * 4,
        scratch_shapes=[
            pltpu.VMEM((slots, size, size), bf16),
            pltpu.VMEM((slots, size, size), bf16),
            pltpu.VMEM((4, height, size), f32),
            pltpu.SemaphoreType.DMA((2, slots // COL_GROUP)),
        ],
        compiler_params=limits(20),
        cost_estimate=cost(400_000_000),
    )(*place, hi, lo, near, far)


def unpack_gram(packed):
    return jnp.concatenate([packed[:, 0:128], packed[:, 128:256]], axis=0)


def pack_gram(gram):
    width = gram.shape[1]
    if width < 128:
        gram = jnp.concatenate([gram, jnp.zeros((16, 128 - width), f32)], axis=1)
    return jnp.concatenate([gram[0:8], gram[8:16]], axis=1)


def eye16():
    return (
        lax.broadcasted_iota(jnp.int32, (16, 16), 0) == lax.broadcasted_iota(jnp.int32, (16, 16), 1)
    ).astype(f32)


def factor_and_inverse(gram):
    work = jnp.concatenate([gram, eye16(), jnp.zeros((16, 96), f32)], axis=1)
    rows = lax.broadcasted_iota(jnp.int32, (16, 128), 0)
    lanes = lax.broadcasted_iota(jnp.int32, (16, 128), 1)
    down = jnp.ones((16, 128), f32)
    across = jnp.ones((16, 128), f32)
    lower = jnp.zeros((16, 128), f32)
    for j in range(16):
        column = jnp.broadcast_to(work[:, j : j + 1], (16, 128))
        pivot = jnp.broadcast_to(column[j : j + 1], (16, 128))
        row = jnp.broadcast_to(work[j : j + 1], (16, 128))
        down = jnp.where(rows == j, pivot, down)
        across = jnp.where(lanes == j, pivot, across)
        lower = jnp.where((lanes == j) & (rows >= j), column, lower)
        work = work - jnp.where(rows > j, column / pivot, 0.0) * row
    lower = lower / jnp.sqrt(across)
    inverse = work / jnp.sqrt(down)
    return lower[:, 0:16], inverse[:, 16:32]


def update_kernel(step, node_total, *refs):
    refs = list(refs)
    take = lambda count: [refs.pop(0) for _ in range(count)]
    (arrived,) = take(1)
    own, one, two, three = take(4)
    before, degree = (None, None) if step == 0 else take(2)
    shift_in = take(1)[0] if step > 1 else None
    (start,) = take(1) if step == 0 else (None,)
    outs = refs
    side = own[...] + one[...] + two[...] + three[...]
    height = arrived.shape[1]
    total = side[0:height]
    for p in range(arrived.shape[0]):
        total = total + arrived[p]
    gram = unpack_gram(side[height : height + 8]) * (1.0 / node_total)
    if step == 0:
        packed, piece_out, state, degree_out, lower_out = outs
        level = total[16:17]
        lower, inverse = factor_and_inverse(gram[:, 0:16])
        block = start[...]
        applied = level * block - total[0:16]
        both = dot_f32(inverse, jnp.concatenate([block, applied], axis=1), ((1,), (0,)))
        degree_out[...] = total[16:24]
        stack = both
        new_vectors = both[:, 0:256]
        new_applied = both[:, 256:512]
        state[...] = both
        basis = new_vectors
        lower_out[...] = lower
    else:
        if step == 1:
            packed, piece_out, state, coeff_out, lower_out, shift_out = outs
        else:
            packed, piece_out, state, coeff_out, lower_out = outs
        width = 16 * step
        coeffs = gram[:, 0:width]
        square = gram[:, width : width + 16]
        square = square - dot_f32(coeffs, coeffs, ((1,), (1,)))
        lower, inverse = factor_and_inverse(square)
        stack = before[...]
        newest = stack[width - 16 : width]
        vectors, applied = newest[:, 0:256], newest[:, 256:512]
        level = degree[0:1]
        twice = level * applied - total[0:16]
        coeff_out[...] = jnp.concatenate([coeffs, jnp.zeros((16, 128 - width), f32)], axis=1)
        if step == 1:
            shift = jnp.broadcast_to(
                jnp.sum(coeffs * eye16(), axis=(0, 1), keepdims=True) * (1.0 / 16), (8, 128)
            )
            shift_out[...] = shift
            scalar = shift[0:1, 0:1]
            moved = applied - scalar * vectors
            twice = twice - scalar * applied - scalar * moved
            coeffs = coeffs - scalar * eye16()
            applied = moved
            stack = jnp.concatenate([vectors, applied], axis=1)
        else:
            scalar = shift_in[0:1, 0:1]
            twice = twice - scalar * applied
            coeff_out[:, width - 16 : width] = coeffs[:, width - 16 : width] + scalar * eye16()
        rest = jnp.concatenate([applied, twice], axis=1) - dot_f32(coeffs, stack, ((1,), (0,)))
        both = dot_f32(inverse, rest, ((1,), (0,)))
        state[0:width] = stack
        state[width : width + 16] = both
        lower_out[...] = lower
        new_applied = both[:, 256:512]
        basis = jnp.concatenate([stack[:, 0:256], both[:, 0:256]], axis=0)
    partial = dot_f32(new_applied, jnp.concatenate([basis, new_applied], axis=0), ((1,), (1,)))
    piece_out[...] = new_applied
    gram_rows = pack_gram(partial)
    if step == ITERS - 1:
        for p in range(packed.shape[0]):
            packed[p] = gram_rows
    else:
        message = jnp.concatenate([new_applied, gram_rows], axis=0)
        for p in range(packed.shape[0]):
            packed[p] = message


def update(step, node_total, arrived, sides, state, degree, shift, start):
    size = arrived.shape[2]
    shapes = [
        jax.ShapeDtypeStruct((8, 8, size) if step == ITERS - 1 else (16, 24, size), f32),
        jax.ShapeDtypeStruct((16, size), f32),
        jax.ShapeDtypeStruct((16 * (step + 1), 2 * size), f32),
    ]
    if step == 0:
        shapes += [jax.ShapeDtypeStruct((8, size), f32), jax.ShapeDtypeStruct((16, 16), f32)]
        extra = [start]
    else:
        shapes += [jax.ShapeDtypeStruct((16, 128), f32), jax.ShapeDtypeStruct((16, 16), f32)]
        extra = [state, degree]
        if step == 1:
            shapes.append(jax.ShapeDtypeStruct((8, 128), f32))
        else:
            extra.append(shift)
    args = [arrived, *sides, *extra]
    return pl.pallas_call(
        functools.partial(update_kernel, step, node_total),
        out_shape=tuple(shapes),
        in_specs=[VMEM] * len(args),
        out_specs=(VMEM,) * len(shapes),
        compiler_params=limits(16),
        cost_estimate=cost(400_000_000),
    )(*args)


def fold_kernel(arrived, packed):
    total = arrived[0]
    for p in range(1, arrived.shape[0]):
        total = total + arrived[p]
    for p in range(packed.shape[0]):
        packed[p] = total


def fold(arrived):
    return pl.pallas_call(
        fold_kernel,
        name="fold",
        out_shape=jax.ShapeDtypeStruct((16, 8, arrived.shape[2]), f32),
        in_specs=[VMEM],
        out_specs=VMEM,
        compiler_params=limits(8),
    )(arrived)


def last_kernel(node_total, arrived, state, shift, *refs):
    coeffs_in, lowers_in = refs[0 : ITERS - 1], refs[ITERS - 1 : 2 * ITERS - 1]
    basis_out, coeffs_out, lowers_out = refs[2 * ITERS - 1 :]
    packed = arrived[0]
    for p in range(1, arrived.shape[0]):
        packed = packed + arrived[p]
    gram = unpack_gram(packed) * (1.0 / node_total)
    width = 16 * ITERS
    coeffs = gram[:, 0:width]
    square = gram[:, width : width + 16] - dot_f32(coeffs, coeffs, ((1,), (1,)))
    stack = state[...]
    rest = stack[width - 16 : width, 256:512] - dot_f32(coeffs, stack[:, 0:256], ((1,), (0,)))
    for k in range(ITERS):
        basis_out[k] = stack[16 * k : 16 * k + 16, 0:256]
        lowers_out[k] = lowers_in[k][...]
        for j in range(ITERS):
            if j > k:
                coeffs_out[k, j] = jnp.zeros((16, 16), f32)
            elif k < ITERS - 1:
                coeffs_out[k, j] = coeffs_in[k][:, 16 * j : 16 * j + 16]
            elif j < k:
                coeffs_out[k, j] = coeffs[:, 16 * j : 16 * j + 16]
            else:
                coeffs_out[k, j] = coeffs[:, 16 * j : 16 * j + 16] + shift[0:1, 0:1] * eye16()
    lower, inverse = factor_and_inverse(square)
    basis_out[ITERS] = dot_f32(inverse, rest, ((1,), (0,)))
    lowers_out[ITERS] = lower


def last(node_total, arrived, state, shift, coeffs, lowers):
    args = [arrived, state, shift, *coeffs, *lowers]
    return pl.pallas_call(
        functools.partial(last_kernel, node_total),
        name="last",
        out_shape=(
            jax.ShapeDtypeStruct((ITERS + 1, 16, arrived.shape[2]), f32),
            jax.ShapeDtypeStruct((ITERS, ITERS, 16, 16), f32),
            jax.ShapeDtypeStruct((ITERS + 1, 16, 16), f32),
        ),
        in_specs=[VMEM] * len(args),
        out_specs=(VMEM,) * 3,
        compiler_params=limits(8),
    )(*args)


def first_message_kernel(block, packed):
    partial = dot_f32(block[...], block[...], ((1,), (1,)))
    message = jnp.concatenate([block[...], pack_gram(partial)], axis=0)
    for p in range(packed.shape[0]):
        packed[p] = message


def first_message(block):
    return pl.pallas_call(
        first_message_kernel,
        name="first_message",
        out_shape=jax.ShapeDtypeStruct((16, 24, block.shape[1]), f32),
        in_specs=[VMEM],
        out_specs=VMEM,
        compiler_params=limits(8),
    )(block)


def shifted(value, hop):
    size = lax.axis_size("grp")
    return lax.ppermute(value, "grp", [(i, (i + hop) % size) for i in range(size)])


def swapped(value):
    return lax.ppermute(value, CORE, [(0, 1), (1, 0)])


def exchanged(value, axes):
    return lax.all_to_all(value, axes, split_axis=0, concat_axis=0, tiled=True)


def body(start_block, tile_values, tile_row, tile_col, tile_count):
    grp_size = lax.axis_size("grp")
    node_total = float(start_block.shape[1] * grp_size * lax.axis_size(COL))
    place = tuple(
        pltpu.with_memory_space_constraint(part, pltpu.MemorySpace.HBM)
        for part in (tile_row, tile_col)
    )
    place = (*place, tile_count)
    start_block = pltpu.with_memory_space_constraint(start_block, pltpu.MemorySpace.HBM)
    tile_values = pltpu.with_memory_space_constraint(tile_values, pltpu.MemorySpace.HBM)
    message = first_message(start_block)
    piece = start_block
    state = degree = shift = hi = lo = None
    lowers, coeffs = [], []
    for step in range(ITERS):
        first = step == 0
        pieces = [piece]
        for hop in range(1, grp_size):
            pieces.append(shifted(piece, hop))
        near = exchanged(message, ZX)
        if first:
            rows, hi, lo = rows_first(place, tile_values, pieces)
            hi = pltpu.with_memory_space_constraint(hi, pltpu.MemorySpace.HBM)
            lo = pltpu.with_memory_space_constraint(lo, pltpu.MemorySpace.HBM)
        else:
            rows = rows_next(place, hi, lo, pieces)
        far = swapped(near)
        arrived = exchanged(rows, COL)
        sides = cols_product(first, place, hi, lo, near, far)
        sides = [sides[0]] + [shifted(sides[hop], hop) for hop in range(1, grp_size)]
        outs = update(step, node_total, arrived, sides, state, degree, shift, start_block)
        message, piece, state = outs[0:3]
        if first:
            degree = outs[3]
        else:
            coeffs.append(outs[3])
        lowers.append(outs[4])
        if step == 1:
            shift = outs[5]
    packed = fold(exchanged(message, ("col_1", "col_2")))
    packed = exchanged(packed, ("grp", "col_0"))
    return last(node_total, packed, state, shift, coeffs, lowers)


def solution(mesh):
    split_mesh = Mesh(
        mesh.devices.reshape(mesh.shape["grp"], 4, 4, 2), ("grp", "col_0", "col_1", "col_2")
    )
    placed = (
        P(None, GRP_COL),
        P("grp", COL, None, None, None),
        P("grp", COL, None),
        P("grp", COL, None),
        P("grp", COL),
    )
    return jax.shard_map(
        body,
        mesh=split_mesh,
        in_specs=placed,
        out_specs=(P(None, None, GRP_COL), P(), P()),
        check_vma=False,
    )
```

```python
import functools
import jax
import jax.numpy as jnp
from jax import lax
from jax.experimental import pallas as pl
from jax.experimental.pallas import tpu as pltpu
from jax.sharding import Mesh
from jax.sharding import PartitionSpec as P

ITERS = 4
ZX = ("col_0", "col_1")
CORE = "col_2"
COL = ("col_0", "col_1", "col_2")
GRP_COL = ("grp", "col_0", "col_1", "col_2")
ROW_GROUP = 8
COL_GROUP = 4
highest = lax.Precision.HIGHEST
VMEM = pl.BlockSpec(memory_space=pltpu.VMEM)
SMEM = pl.BlockSpec(memory_space=pltpu.SMEM)
HBM = pl.BlockSpec(memory_space=pltpu.MemorySpace.HBM)
MIB = 1 << 20
f32 = jnp.float32
bf16 = jnp.bfloat16


def split(x):
    hi = x.astype(bf16)
    return hi, (x - hi.astype(f32)).astype(bf16)


def dot(a, b, dims):
    return lax.dot_general(a, b, (dims, ((), ())), preferred_element_type=f32)


def dot_f32(a, b, dims):
    return lax.dot_general(a, b, (dims, ((), ())), precision=highest, preferred_element_type=f32)


def limits(mib):
    return pltpu.CompilerParams(vmem_limit_bytes=mib * MIB)


def cost(flops):
    return pl.CostEstimate(flops=flops, bytes_accessed=MIB, transcendentals=0)


def products(lhs_hi, lhs_lo, hi, lo, dims, first, live):
    top = dot(lhs_hi, hi, dims)
    low = dot(lhs_lo, lo, dims)
    out = top[0:16] + top[16:32] + low[0:16]
    if first:
        out = jnp.concatenate([out, top[32:40] + low[16:24]], axis=0)
    return out * live


def stacked_lhs(piece, first):
    hi, lo = split(piece)
    if first:
        ones = jnp.ones((16, piece.shape[1]), bf16)
        return jnp.concatenate([hi, lo, ones], axis=0), jnp.concatenate([hi, ones], axis=0)
    return jnp.concatenate([hi, lo], axis=0), hi


def fill_pieces(pieces, lhs_hi, lhs_lo, first):
    for k, piece in enumerate(pieces):
        lhs_hi[k], lhs_lo[k] = stacked_lhs(piece[...], first)


def group_rows(base, place, lhs_hi, lhs_lo, hi, lo, out, first):
    tile_row, tile_col, tile_count = place
    results = []
    for u in range(ROW_GROUP):
        s = base + u
        k = ((tile_row[0, 0, 0] >> 5) - (tile_col[0, 0, s] >> 5)) & 3
        live = (s < tile_count[0, 0]).astype(f32)
        results.append(
            products(lhs_hi[k], lhs_lo[k], hi[s], lo[s], ((1,), (1,)), first, live)
        )
    for u in range(ROW_GROUP):
        out[tile_row[0, 0, base + u] & 31] += results[u]


def groups_of(tile_count, group):
    return (tile_count[0, 0] + (group - 1)) // group


def group_copies(q, group, source_hi, source_lo, hi, lo, sems):
    part = pl.ds(q * group, group)
    return (
        pltpu.make_async_copy(source_hi.at[part], hi.at[part], sems.at[0, q]),
        pltpu.make_async_copy(source_lo.at[part], lo.at[part], sems.at[1, q]),
    )


def start_groups(tile_count, group, index_copies, *refs):
    for copy in group_copies(0, group, *refs):
        copy.start()
    for copy in index_copies:
        copy.start()

    @pl.loop(1, groups_of(tile_count, group))
    def _(q):
        for copy in group_copies(q, group, *refs):
            copy.start()


def index_fetch(row_in, col_in, tile_row, tile_col, sems):
    return (
        pltpu.make_async_copy(row_in, tile_row, sems.at[0]),
        pltpu.make_async_copy(col_in, tile_col, sems.at[1]),
    )


def rows_first_kernel(
    row_in, col_in, tile_count, tiles, own, one, two, three, out, hi_out, lo_out,
    buf, hi, lo, lhs_hi, lhs_lo, tile_row, tile_col, sems, out_sems, index_sems
):
    group = ROW_GROUP
    count = groups_of(tile_count, group)

    def arriving(q):
        part = pl.ds(q * group, group)
        return pltpu.make_async_copy(tiles.at[0, 0, part], buf.at[part], sems.at[q])

    arriving(0).start()
    index_copies = index_fetch(row_in, col_in, tile_row, tile_col, index_sems)
    for copy in index_copies:
        copy.start()

    @pl.loop(1, count)
    def _(q):
        arriving(q).start()

    fill_pieces((own, one, two, three), lhs_hi, lhs_lo, True)
    out[...] = jnp.zeros_like(out)
    for copy in index_copies:
        copy.wait()

    @pl.loop(0, count)
    def _(q):
        arriving(q).wait()
        for u in range(group):
            s = q * group + u
            hi[s], lo[s] = split(buf[s])
        for copy in group_copies(q, group, hi, lo, hi_out, lo_out, out_sems):
            copy.start()
        group_rows(
            q * group, (tile_row, tile_col, tile_count), lhs_hi, lhs_lo, hi, lo, out, True
        )

    @pl.loop(0, count)
    def _(q):
        for copy in group_copies(q, group, hi, lo, hi_out, lo_out, out_sems):
            copy.wait()


def rows_next_kernel(
    row_in, col_in, tile_count, hi_in, lo_in, own, one, two, three, out,
    hi, lo, lhs_hi, lhs_lo, tile_row, tile_col, sems, index_sems
):
    group = ROW_GROUP
    index_copies = index_fetch(row_in, col_in, tile_row, tile_col, index_sems)
    start_groups(tile_count, group, index_copies, hi_in, lo_in, hi, lo, sems)
    fill_pieces((own, one, two, three), lhs_hi, lhs_lo, False)
    out[...] = jnp.zeros_like(out)
    for copy in index_copies:
        copy.wait()

    @pl.loop(0, groups_of(tile_count, group))
    def _(q):
        for copy in group_copies(q, group, hi_in, lo_in, hi, lo, sems):
            copy.wait()
        group_rows(q * group, (tile_row, tile_col, tile_count), lhs_hi, lhs_lo, hi, lo, out, False)


def cols_kernel(
    first, row_in, col_in, tile_count, hi_in, lo_in, near, far, own, one, two, three,
    hi, lo, acc, tile_row, tile_col, sems, index_sems
):
    group = COL_GROUP
    index_copies = index_fetch(row_in, col_in, tile_row, tile_col, index_sems)
    start_groups(tile_count, group, index_copies, hi_in, lo_in, hi, lo, sems)
    acc[...] = jnp.zeros_like(acc)
    if first:
        total = jnp.zeros((16, 16), f32)
        for part in (near, far):
            for p in range(part.shape[0]):
                total = total + dot_f32(part[p], part[p], ((1,), (1,)))
        gram = pack_gram(total)
    else:
        gram = jnp.zeros_like(near[0, 16:24])
        for p in range(near.shape[0]):
            gram = gram + (near[p, 16:24] + far[p, 16:24])
    for copy in index_copies:
        copy.wait()

    @pl.loop(0, groups_of(tile_count, group))
    def _(q):
        for copy in group_copies(q, group, hi_in, lo_in, hi, lo, sems):
            copy.wait()
        results, slots = [], []
        for u in range(group):
            s = q * group + u
            row = tile_row[0, 0, s] & 31
            place = row >> 1
            same = ((row ^ tile_col[0, 0, 0]) & 1) == 0
            piece = jnp.where(same, near[place, 0:16], far[place, 0:16])
            left_hi, left_lo = stacked_lhs(piece, first)
            live = (s < tile_count[0, 0]).astype(f32)
            results.append(
                products(left_hi, left_lo, hi[s], lo[s], ((1,), (0,)), first, live)
            )
            slots.append(((tile_col[0, 0, s] >> 5) - (tile_row[0, 0, 0] >> 5)) & 3)
        for u in range(group):
            acc[slots[u]] += results[u]

    for k, out in enumerate((own, one, two, three)):
        out[...] = jnp.concatenate([acc[k], gram], axis=0)


def rows_first(place, tiles, pieces):
    slots, size = tiles.shape[2], tiles.shape[3]
    return pl.pallas_call(
        rows_first_kernel,
        name="rows_first",
        out_shape=(
            jax.ShapeDtypeStruct((32, 24, size), f32),
            pltpu.MemorySpace.HBM((slots, size, size), bf16),
            pltpu.MemorySpace.HBM((slots, size, size), bf16),
        ),
        in_specs=[HBM, HBM, SMEM] + [HBM] + [VMEM] * 4,
        out_specs=(VMEM, HBM, HBM),
        scratch_shapes=[
            pltpu.VMEM((slots, size, size), f32),
            pltpu.VMEM((slots, size, size), bf16),
            pltpu.VMEM((slots, size, size), bf16),
            pltpu.VMEM((4, 48, size), bf16),
            pltpu.VMEM((4, 32, size), bf16),
            pltpu.SMEM((1, 1, slots), jnp.int32),
            pltpu.SMEM((1, 1, slots), jnp.int32),
            pltpu.SemaphoreType.DMA((slots // ROW_GROUP,)),
            pltpu.SemaphoreType.DMA((2, slots // ROW_GROUP)),
            pltpu.SemaphoreType.DMA((2,)),
        ],
        compiler_params=limits(28),
        cost_estimate=cost(400_000_000),
    )(*place, tiles, *pieces)


def rows_next(place, hi, lo, pieces):
    slots, size = hi.shape[0], hi.shape[1]
    return pl.pallas_call(
        rows_next_kernel,
        name="rows_next",
        out_shape=jax.ShapeDtypeStruct((32, 16, size), f32),
        in_specs=[HBM, HBM, SMEM] + [HBM] * 2 + [VMEM] * 4,
        out_specs=VMEM,
        scratch_shapes=[
            pltpu.VMEM((slots, size, size), bf16),
            pltpu.VMEM((slots, size, size), bf16),
            pltpu.VMEM((4, 32, size), bf16),
            pltpu.VMEM((4, 16, size), bf16),
            pltpu.SMEM((1, 1, slots), jnp.int32),
            pltpu.SMEM((1, 1, slots), jnp.int32),
            pltpu.SemaphoreType.DMA((2, slots // ROW_GROUP)),
            pltpu.SemaphoreType.DMA((2,)),
        ],
        compiler_params=limits(20),
        cost_estimate=cost(400_000_000),
    )(*place, hi, lo, *pieces)


def cols_product(first, place, hi, lo, near, far):
    height = 24 if first else 16
    slots, size = hi.shape[0], hi.shape[1]
    out = jax.ShapeDtypeStruct((height + 8, size), f32)
    return pl.pallas_call(
        functools.partial(cols_kernel, first),
        name="cols_first" if first else "cols_next",
        out_shape=(out,) * 4,
        in_specs=[HBM, HBM, SMEM] + [HBM] * 2 + [VMEM] * 2,
        out_specs=(VMEM,) * 4,
        scratch_shapes=[
            pltpu.VMEM((slots, size, size), bf16),
            pltpu.VMEM((slots, size, size), bf16),
            pltpu.VMEM((4, height, size), f32),
            pltpu.SMEM((1, 1, slots), jnp.int32),
            pltpu.SMEM((1, 1, slots), jnp.int32),
            pltpu.SemaphoreType.DMA((2, slots // COL_GROUP)),
            pltpu.SemaphoreType.DMA((2,)),
        ],
        compiler_params=limits(20),
        cost_estimate=cost(400_000_000),
    )(*place, hi, lo, near, far)


def unpack_gram(packed):
    return jnp.concatenate([packed[:, 0:128], packed[:, 128:256]], axis=0)


def pack_gram(gram):
    width = gram.shape[1]
    if width < 128:
        gram = jnp.concatenate([gram, jnp.zeros((16, 128 - width), f32)], axis=1)
    return jnp.concatenate([gram[0:8], gram[8:16]], axis=1)


def eye16():
    return (
        lax.broadcasted_iota(jnp.int32, (16, 16), 0) == lax.broadcasted_iota(jnp.int32, (16, 16), 1)
    ).astype(f32)


def factor_and_inverse(gram):
    work = jnp.concatenate([gram, eye16(), jnp.zeros((16, 96), f32)], axis=1)
    rows = lax.broadcasted_iota(jnp.int32, (16, 128), 0)
    lanes = lax.broadcasted_iota(jnp.int32, (16, 128), 1)
    down = jnp.ones((16, 128), f32)
    across = jnp.ones((16, 128), f32)
    lower = jnp.zeros((16, 128), f32)
    for j in range(16):
        column = jnp.broadcast_to(work[:, j : j + 1], (16, 128))
        pivot = jnp.broadcast_to(column[j : j + 1], (16, 128))
        row = jnp.broadcast_to(work[j : j + 1], (16, 128))
        down = jnp.where(rows == j, pivot, down)
        across = jnp.where(lanes == j, pivot, across)
        lower = jnp.where((lanes == j) & (rows >= j), column, lower)
        work = work - jnp.where(rows > j, column / pivot, 0.0) * row
    lower = lower / jnp.sqrt(across)
    inverse = work / jnp.sqrt(down)
    return lower[:, 0:16], inverse[:, 16:32]


def update_kernel(step, node_total, *refs):
    refs = list(refs)
    take = lambda count: [refs.pop(0) for _ in range(count)]
    (arrived,) = take(1)
    own, one, two, three = take(4)
    before, degree = (None, None) if step == 0 else take(2)
    shift_in = take(1)[0] if step > 1 else None
    (start,) = take(1) if step == 0 else (None,)
    outs = refs
    side = own[...] + one[...] + two[...] + three[...]
    height = arrived.shape[1]
    total = side[0:height]
    for p in range(arrived.shape[0]):
        total = total + arrived[p]
    gram = unpack_gram(side[height : height + 8]) * (1.0 / node_total)
    if step == 0:
        packed, piece_out, state, degree_out, lower_out = outs
        level = total[16:17]
        lower, inverse = factor_and_inverse(gram[:, 0:16])
        block = start[...]
        applied = level * block - total[0:16]
        both = dot_f32(inverse, jnp.concatenate([block, applied], axis=1), ((1,), (0,)))
        degree_out[...] = total[16:24]
        stack = both
        new_vectors = both[:, 0:256]
        new_applied = both[:, 256:512]
        state[...] = both
        basis = new_vectors
        lower_out[...] = lower
    else:
        if step == 1:
            packed, piece_out, state, coeff_out, lower_out, shift_out = outs
        else:
            packed, piece_out, state, coeff_out, lower_out = outs
        width = 16 * step
        coeffs = gram[:, 0:width]
        square = gram[:, width : width + 16]
        square = square - dot_f32(coeffs, coeffs, ((1,), (1,)))
        lower, inverse = factor_and_inverse(square)
        stack = before[...]
        newest = stack[width - 16 : width]
        vectors, applied = newest[:, 0:256], newest[:, 256:512]
        level = degree[0:1]
        twice = level * applied - total[0:16]
        coeff_out[...] = jnp.concatenate([coeffs, jnp.zeros((16, 128 - width), f32)], axis=1)
        if step == 1:
            shift = jnp.broadcast_to(
                jnp.sum(coeffs * eye16(), axis=(0, 1), keepdims=True) * (1.0 / 16), (8, 128)
            )
            shift_out[...] = shift
            scalar = shift[0:1, 0:1]
            moved = applied - scalar * vectors
            twice = twice - scalar * applied - scalar * moved
            coeffs = coeffs - scalar * eye16()
            applied = moved
            stack = jnp.concatenate([vectors, applied], axis=1)
        else:
            scalar = shift_in[0:1, 0:1]
            twice = twice - scalar * applied
            coeff_out[:, width - 16 : width] = coeffs[:, width - 16 : width] + scalar * eye16()
        rest = jnp.concatenate([applied, twice], axis=1) - dot_f32(coeffs, stack, ((1,), (0,)))
        both = dot_f32(inverse, rest, ((1,), (0,)))
        state[0:width] = stack
        state[width : width + 16] = both
        lower_out[...] = lower
        new_applied = both[:, 256:512]
        basis = jnp.concatenate([stack[:, 0:256], both[:, 0:256]], axis=0)
    partial = dot_f32(new_applied, jnp.concatenate([basis, new_applied], axis=0), ((1,), (1,)))
    piece_out[...] = new_applied
    gram_rows = pack_gram(partial)
    if step == ITERS - 1:
        for p in range(packed.shape[0]):
            packed[p] = gram_rows
    else:
        message = jnp.concatenate([new_applied, gram_rows], axis=0)
        for p in range(packed.shape[0]):
            packed[p] = message


def update(step, node_total, arrived, sides, state, degree, shift, start):
    size = arrived.shape[2]
    shapes = [
        jax.ShapeDtypeStruct((8, 8, size) if step == ITERS - 1 else (16, 24, size), f32),
        jax.ShapeDtypeStruct((16, size), f32),
        jax.ShapeDtypeStruct((16 * (step + 1), 2 * size), f32),
    ]
    if step == 0:
        shapes += [jax.ShapeDtypeStruct((8, size), f32), jax.ShapeDtypeStruct((16, 16), f32)]
        extra = [start]
    else:
        shapes += [jax.ShapeDtypeStruct((16, 128), f32), jax.ShapeDtypeStruct((16, 16), f32)]
        extra = [state, degree]
        if step == 1:
            shapes.append(jax.ShapeDtypeStruct((8, 128), f32))
        else:
            extra.append(shift)
    args = [arrived, *sides, *extra]
    return pl.pallas_call(
        functools.partial(update_kernel, step, node_total),
        out_shape=tuple(shapes),
        in_specs=[VMEM] * len(args),
        out_specs=(VMEM,) * len(shapes),
        compiler_params=limits(16),
        cost_estimate=cost(400_000_000),
    )(*args)


def fold_kernel(arrived, packed):
    total = arrived[0]
    for p in range(1, arrived.shape[0]):
        total = total + arrived[p]
    for p in range(packed.shape[0]):
        packed[p] = total


def fold(arrived):
    return pl.pallas_call(
        fold_kernel,
        name="fold",
        out_shape=jax.ShapeDtypeStruct((16, 8, arrived.shape[2]), f32),
        in_specs=[VMEM],
        out_specs=VMEM,
        compiler_params=limits(8),
    )(arrived)


def last_kernel(node_total, arrived, state, shift, *refs):
    coeffs_in, lowers_in = refs[0 : ITERS - 1], refs[ITERS - 1 : 2 * ITERS - 1]
    basis_out, coeffs_out, lowers_out = refs[2 * ITERS - 1 :]
    packed = arrived[0]
    for p in range(1, arrived.shape[0]):
        packed = packed + arrived[p]
    gram = unpack_gram(packed) * (1.0 / node_total)
    width = 16 * ITERS
    coeffs = gram[:, 0:width]
    square = gram[:, width : width + 16] - dot_f32(coeffs, coeffs, ((1,), (1,)))
    stack = state[...]
    rest = stack[width - 16 : width, 256:512] - dot_f32(coeffs, stack[:, 0:256], ((1,), (0,)))
    for k in range(ITERS):
        basis_out[k] = stack[16 * k : 16 * k + 16, 0:256]
        lowers_out[k] = lowers_in[k][...]
        for j in range(ITERS):
            if j > k:
                coeffs_out[k, j] = jnp.zeros((16, 16), f32)
            elif k < ITERS - 1:
                coeffs_out[k, j] = coeffs_in[k][:, 16 * j : 16 * j + 16]
            elif j < k:
                coeffs_out[k, j] = coeffs[:, 16 * j : 16 * j + 16]
            else:
                coeffs_out[k, j] = coeffs[:, 16 * j : 16 * j + 16] + shift[0:1, 0:1] * eye16()
    lower, inverse = factor_and_inverse(square)
    basis_out[ITERS] = dot_f32(inverse, rest, ((1,), (0,)))
    lowers_out[ITERS] = lower


def last(node_total, arrived, state, shift, coeffs, lowers):
    args = [arrived, state, shift, *coeffs, *lowers]
    return pl.pallas_call(
        functools.partial(last_kernel, node_total),
        name="last",
        out_shape=(
            jax.ShapeDtypeStruct((ITERS + 1, 16, arrived.shape[2]), f32),
            jax.ShapeDtypeStruct((ITERS, ITERS, 16, 16), f32),
            jax.ShapeDtypeStruct((ITERS + 1, 16, 16), f32),
        ),
        in_specs=[VMEM] * len(args),
        out_specs=(VMEM,) * 3,
        compiler_params=limits(8),
    )(*args)


def shifted(value, hop):
    size = lax.axis_size("grp")
    return lax.ppermute(value, "grp", [(i, (i + hop) % size) for i in range(size)])


def swapped(value):
    return lax.ppermute(value, CORE, [(0, 1), (1, 0)])


def exchanged(value, axes):
    return lax.all_to_all(value, axes, split_axis=0, concat_axis=0, tiled=True)


def body(start_block, tile_values, tile_row, tile_col, tile_count):
    grp_size = lax.axis_size("grp")
    node_total = float(start_block.shape[1] * grp_size * lax.axis_size(COL))
    message = jnp.broadcast_to(start_block, (lax.axis_size(ZX), *start_block.shape))
    place = tuple(
        pltpu.with_memory_space_constraint(part, pltpu.MemorySpace.HBM)
        for part in (tile_row, tile_col)
    )
    place = (*place, tile_count)
    start_block = pltpu.with_memory_space_constraint(start_block, pltpu.MemorySpace.HBM)
    tile_values = pltpu.with_memory_space_constraint(tile_values, pltpu.MemorySpace.HBM)
    piece = start_block
    state = degree = shift = hi = lo = None
    lowers, coeffs = [], []
    for step in range(ITERS):
        first = step == 0
        pieces = [piece]
        for hop in range(1, grp_size):
            pieces.append(shifted(piece, hop))
        near = exchanged(message, ZX)
        if first:
            rows, hi, lo = rows_first(place, tile_values, pieces)
            hi = pltpu.with_memory_space_constraint(hi, pltpu.MemorySpace.HBM)
            lo = pltpu.with_memory_space_constraint(lo, pltpu.MemorySpace.HBM)
        else:
            rows = rows_next(place, hi, lo, pieces)
        far = swapped(near)
        arrived = exchanged(rows, COL)
        sides = cols_product(first, place, hi, lo, near, far)
        sides = [sides[0]] + [shifted(sides[hop], hop) for hop in range(1, grp_size)]
        outs = update(step, node_total, arrived, sides, state, degree, shift, start_block)
        message, piece, state = outs[0:3]
        if first:
            degree = outs[3]
        else:
            coeffs.append(outs[3])
        lowers.append(outs[4])
        if step == 1:
            shift = outs[5]
    packed = fold(exchanged(message, ("col_1", "col_2")))
    packed = exchanged(packed, ("grp", "col_0"))
    return last(node_total, packed, state, shift, coeffs, lowers)


def solution(mesh):
    split_mesh = Mesh(
        mesh.devices.reshape(mesh.shape["grp"], 4, 4, 2), ("grp", "col_0", "col_1", "col_2")
    )
    placed = (
        P(None, GRP_COL),
        P("grp", COL, None, None, None),
        P("grp", COL, None),
        P("grp", COL, None),
        P("grp", COL),
    )
    return jax.shard_map(
        body,
        mesh=split_mesh,
        in_specs=placed,
        out_specs=(P(None, None, GRP_COL), P(), P()),
        check_vma=False,
    )
```

```python
import functools
import jax
import jax.numpy as jnp
from jax import lax
from jax.experimental import pallas as pl
from jax.experimental.pallas import tpu as pltpu
from jax.sharding import Mesh
from jax.sharding import PartitionSpec as P

ITERS = 4
ZX = ("col_0", "col_1")
CORE = "col_2"
COL = ("col_0", "col_1", "col_2")
GRP_COL = ("grp", "col_0", "col_1", "col_2")
ROW_GROUP = 8
COL_GROUP = 4
FACTOR_GROUP = 8
highest = lax.Precision.HIGHEST
VMEM = pl.BlockSpec(memory_space=pltpu.VMEM)
SMEM = pl.BlockSpec(memory_space=pltpu.SMEM)
HBM = pl.BlockSpec(memory_space=pltpu.MemorySpace.HBM)
MIB = 1 << 20
f32 = jnp.float32
bf16 = jnp.bfloat16


def split(x):
    hi = x.astype(bf16)
    return hi, (x - hi.astype(f32)).astype(bf16)


def dot(a, b, dims):
    return lax.dot_general(a, b, (dims, ((), ())), preferred_element_type=f32)


def dot_f32(a, b, dims):
    return lax.dot_general(a, b, (dims, ((), ())), precision=highest, preferred_element_type=f32)


def limits(mib):
    return pltpu.CompilerParams(vmem_limit_bytes=mib * MIB)


def cost(flops):
    return pl.CostEstimate(flops=flops, bytes_accessed=MIB, transcendentals=0)


def products(lhs_hi, lhs_lo, hi, lo, dims, first, live):
    top = dot(lhs_hi, hi, dims)
    low = dot(lhs_lo, lo, dims)
    out = top[0:16] + top[16:32] + low[0:16]
    if first:
        out = jnp.concatenate([out, top[32:40] + low[16:24]], axis=0)
    return out * live


def stacked_lhs(piece, first):
    hi, lo = split(piece)
    if first:
        ones = jnp.ones((16, piece.shape[1]), bf16)
        return jnp.concatenate([hi, lo, ones], axis=0), jnp.concatenate([hi, ones], axis=0)
    return jnp.concatenate([hi, lo], axis=0), hi


def fill_pieces(pieces, lhs_hi, lhs_lo, first):
    for k, piece in enumerate(pieces):
        lhs_hi[k], lhs_lo[k] = stacked_lhs(piece[...], first)


def group_rows(base, place, lhs_hi, lhs_lo, hi, lo, out, first):
    tile_row, tile_col, tile_count = place
    results = []
    for u in range(ROW_GROUP):
        s = base + u
        k = ((tile_row[0, 0, 0] >> 5) - (tile_col[0, 0, s] >> 5)) & 3
        live = (s < tile_count[0, 0]).astype(f32)
        results.append(
            products(lhs_hi[k], lhs_lo[k], hi[s], lo[s], ((1,), (1,)), first, live)
        )
    for u in range(ROW_GROUP):
        out[tile_row[0, 0, base + u] & 31] += results[u]


def groups_of(tile_count, group):
    return (tile_count[0, 0] + (group - 1)) // group


def group_copies(q, group, source_hi, source_lo, hi, lo, sems):
    part = pl.ds(q * group, group)
    return (
        pltpu.make_async_copy(source_hi.at[part], hi.at[part], sems.at[0, q]),
        pltpu.make_async_copy(source_lo.at[part], lo.at[part], sems.at[1, q]),
    )


def start_groups(tile_count, group, index_copies, *refs):
    for copy in group_copies(0, group, *refs):
        copy.start()
    for copy in index_copies:
        copy.start()

    @pl.loop(1, groups_of(tile_count, group))
    def _(q):
        for copy in group_copies(q, group, *refs):
            copy.start()


def index_fetch(row_in, col_in, tile_row, tile_col, sems):
    return (
        pltpu.make_async_copy(row_in, tile_row, sems.at[0]),
        pltpu.make_async_copy(col_in, tile_col, sems.at[1]),
    )


def rows_first_kernel(
    row_in, col_in, tile_count, tiles, own, one, two, three, out, hi_out, lo_out,
    buf, hi, lo, lhs_hi, lhs_lo, tile_row, tile_col, sems, out_sems, index_sems
):
    group = ROW_GROUP
    count = groups_of(tile_count, group)

    def arriving(q):
        part = pl.ds(q * group, group)
        return pltpu.make_async_copy(tiles.at[0, 0, part], buf.at[part], sems.at[q])

    arriving(0).start()
    index_copies = index_fetch(row_in, col_in, tile_row, tile_col, index_sems)
    for copy in index_copies:
        copy.start()

    @pl.loop(1, count)
    def _(q):
        arriving(q).start()

    fill_pieces((own, one, two, three), lhs_hi, lhs_lo, True)
    out[...] = jnp.zeros_like(out)
    for copy in index_copies:
        copy.wait()

    @pl.loop(0, count)
    def _(q):
        arriving(q).wait()
        for u in range(group):
            s = q * group + u
            hi[s], lo[s] = split(buf[s])
        for copy in group_copies(q, group, hi, lo, hi_out, lo_out, out_sems):
            copy.start()
        group_rows(
            q * group, (tile_row, tile_col, tile_count), lhs_hi, lhs_lo, hi, lo, out, True
        )

    @pl.loop(0, count)
    def _(q):
        for copy in group_copies(q, group, hi, lo, hi_out, lo_out, out_sems):
            copy.wait()


def rows_next_kernel(
    row_in, col_in, tile_count, hi_in, lo_in, own, one, two, three, out,
    hi, lo, lhs_hi, lhs_lo, tile_row, tile_col, sems, index_sems
):
    group = ROW_GROUP
    index_copies = index_fetch(row_in, col_in, tile_row, tile_col, index_sems)
    start_groups(tile_count, group, index_copies, hi_in, lo_in, hi, lo, sems)
    fill_pieces((own, one, two, three), lhs_hi, lhs_lo, False)
    out[...] = jnp.zeros_like(out)
    for copy in index_copies:
        copy.wait()

    @pl.loop(0, groups_of(tile_count, group))
    def _(q):
        for copy in group_copies(q, group, hi_in, lo_in, hi, lo, sems):
            copy.wait()
        group_rows(q * group, (tile_row, tile_col, tile_count), lhs_hi, lhs_lo, hi, lo, out, False)


def cols_kernel(
    first, row_in, col_in, tile_count, hi_in, lo_in, near, far, own, one, two, three,
    hi, lo, acc, tile_row, tile_col, sems, index_sems
):
    group = COL_GROUP
    index_copies = index_fetch(row_in, col_in, tile_row, tile_col, index_sems)
    start_groups(tile_count, group, index_copies, hi_in, lo_in, hi, lo, sems)
    acc[...] = jnp.zeros_like(acc)
    if first:
        total = jnp.zeros((16, 16), f32)
        for part in (near, far):
            for p in range(part.shape[0]):
                total = total + dot_f32(part[p], part[p], ((1,), (1,)))
        gram = pack_gram(total)
    else:
        gram = jnp.zeros_like(near[0, 16:24])
        for p in range(near.shape[0]):
            gram = gram + (near[p, 16:24] + far[p, 16:24])
    for copy in index_copies:
        copy.wait()

    @pl.loop(0, groups_of(tile_count, group))
    def _(q):
        for copy in group_copies(q, group, hi_in, lo_in, hi, lo, sems):
            copy.wait()
        results, slots = [], []
        for u in range(group):
            s = q * group + u
            row = tile_row[0, 0, s] & 31
            place = row >> 1
            same = ((row ^ tile_col[0, 0, 0]) & 1) == 0
            piece = jnp.where(same, near[place, 0:16], far[place, 0:16])
            left_hi, left_lo = stacked_lhs(piece, first)
            live = (s < tile_count[0, 0]).astype(f32)
            results.append(
                products(left_hi, left_lo, hi[s], lo[s], ((1,), (0,)), first, live)
            )
            slots.append(((tile_col[0, 0, s] >> 5) - (tile_row[0, 0, 0] >> 5)) & 3)
        for u in range(group):
            acc[slots[u]] += results[u]

    for k, out in enumerate((own, one, two, three)):
        out[...] = jnp.concatenate([acc[k], gram], axis=0)


def rows_first(place, tiles, pieces):
    slots, size = tiles.shape[2], tiles.shape[3]
    return pl.pallas_call(
        rows_first_kernel,
        name="rows_first",
        out_shape=(
            jax.ShapeDtypeStruct((32, 24, size), f32),
            pltpu.MemorySpace.HBM((slots, size, size), bf16),
            pltpu.MemorySpace.HBM((slots, size, size), bf16),
        ),
        in_specs=[HBM, HBM, SMEM] + [HBM] + [VMEM] * 4,
        out_specs=(VMEM, HBM, HBM),
        scratch_shapes=[
            pltpu.VMEM((slots, size, size), f32),
            pltpu.VMEM((slots, size, size), bf16),
            pltpu.VMEM((slots, size, size), bf16),
            pltpu.VMEM((4, 48, size), bf16),
            pltpu.VMEM((4, 32, size), bf16),
            pltpu.SMEM((1, 1, slots), jnp.int32),
            pltpu.SMEM((1, 1, slots), jnp.int32),
            pltpu.SemaphoreType.DMA((slots // ROW_GROUP,)),
            pltpu.SemaphoreType.DMA((2, slots // ROW_GROUP)),
            pltpu.SemaphoreType.DMA((2,)),
        ],
        compiler_params=limits(28),
        cost_estimate=cost(400_000_000),
    )(*place, tiles, *pieces)


def rows_next(place, hi, lo, pieces):
    slots, size = hi.shape[0], hi.shape[1]
    return pl.pallas_call(
        rows_next_kernel,
        name="rows_next",
        out_shape=jax.ShapeDtypeStruct((32, 16, size), f32),
        in_specs=[HBM, HBM, SMEM] + [HBM] * 2 + [VMEM] * 4,
        out_specs=VMEM,
        scratch_shapes=[
            pltpu.VMEM((slots, size, size), bf16),
            pltpu.VMEM((slots, size, size), bf16),
            pltpu.VMEM((4, 32, size), bf16),
            pltpu.VMEM((4, 16, size), bf16),
            pltpu.SMEM((1, 1, slots), jnp.int32),
            pltpu.SMEM((1, 1, slots), jnp.int32),
            pltpu.SemaphoreType.DMA((2, slots // ROW_GROUP)),
            pltpu.SemaphoreType.DMA((2,)),
        ],
        compiler_params=limits(20),
        cost_estimate=cost(400_000_000),
    )(*place, hi, lo, *pieces)


def cols_product(first, place, hi, lo, near, far):
    height = 24 if first else 16
    slots, size = hi.shape[0], hi.shape[1]
    out = jax.ShapeDtypeStruct((height + 8, size), f32)
    return pl.pallas_call(
        functools.partial(cols_kernel, first),
        name="cols_first" if first else "cols_next",
        out_shape=(out,) * 4,
        in_specs=[HBM, HBM, SMEM] + [HBM] * 2 + [VMEM] * 2,
        out_specs=(VMEM,) * 4,
        scratch_shapes=[
            pltpu.VMEM((slots, size, size), bf16),
            pltpu.VMEM((slots, size, size), bf16),
            pltpu.VMEM((4, height, size), f32),
            pltpu.SMEM((1, 1, slots), jnp.int32),
            pltpu.SMEM((1, 1, slots), jnp.int32),
            pltpu.SemaphoreType.DMA((2, slots // COL_GROUP)),
            pltpu.SemaphoreType.DMA((2,)),
        ],
        compiler_params=limits(20),
        cost_estimate=cost(400_000_000),
    )(*place, hi, lo, near, far)


def unpack_gram(packed):
    return jnp.concatenate([packed[:, 0:128], packed[:, 128:256]], axis=0)


def pack_gram(gram):
    width = gram.shape[1]
    if width < 128:
        gram = jnp.concatenate([gram, jnp.zeros((16, 128 - width), f32)], axis=1)
    return jnp.concatenate([gram[0:8], gram[8:16]], axis=1)


def eye16():
    return (
        lax.broadcasted_iota(jnp.int32, (16, 16), 0) == lax.broadcasted_iota(jnp.int32, (16, 16), 1)
    ).astype(f32)


def factor_and_inverse(gram):
    work = jnp.concatenate([gram, eye16(), jnp.zeros((16, 96), f32)], axis=1)
    rows = lax.broadcasted_iota(jnp.int32, (16, 128), 0)
    lanes = lax.broadcasted_iota(jnp.int32, (16, 128), 1)
    down = jnp.ones((16, 128), f32)
    across = jnp.ones((16, 128), f32)
    lower = jnp.zeros((16, 128), f32)

    def half(x):
        return jnp.broadcast_to(x, (8, 128))

    def full(x):
        return jnp.concatenate([x, x], axis=0)

    for base in range(0, 16, FACTOR_GROUP):
        group = range(FACTOR_GROUP)
        columns = [jnp.broadcast_to(work[:, base + i : base + i + 1], (16, 128)) for i in group]
        across_rows = [half(work[base + i : base + i + 1]) for i in group]
        corner = {
            (i, k): half(work[base + i : base + i + 1, base + k : base + k + 1])
            for i in group
            for k in range(i + 1)
        }
        scaled = []
        for i in group:
            pivot = corner[i, i]
            inverse = 1.0 / pivot
            for k in range(i + 1, FACTOR_GROUP):
                ratio = corner[k, i] * inverse
                columns[k] = columns[k] - columns[i] * full(ratio)
                across_rows[k] = across_rows[k] - across_rows[i] * ratio
                for m in range(k, FACTOR_GROUP):
                    corner[m, k] = corner[m, k] - ratio * corner[m, i]
            scaled.append(across_rows[i] * inverse)
            at = base + i
            down = jnp.where(rows == at, full(pivot), down)
            across = jnp.where(lanes == at, full(pivot), across)
            lower = jnp.where((lanes == at) & (rows >= at), columns[i], lower)
        for i in group:
            work = work - jnp.where(rows > base + i, columns[i], 0.0) * full(scaled[i])
    lower = lower / jnp.sqrt(across)
    inverse = work / jnp.sqrt(down)
    return lower[:, 0:16], inverse[:, 16:32]


def update_kernel(step, node_total, *refs):
    refs = list(refs)
    take = lambda count: [refs.pop(0) for _ in range(count)]
    (arrived,) = take(1)
    own, one, two, three = take(4)
    before, degree = (None, None) if step == 0 else take(2)
    shift_in = take(1)[0] if step > 1 else None
    (start,) = take(1) if step == 0 else (None,)
    outs = refs
    side = own[...] + one[...] + two[...] + three[...]
    height = arrived.shape[1]
    total = side[0:height]
    for p in range(arrived.shape[0]):
        total = total + arrived[p]
    gram = unpack_gram(side[height : height + 8]) * (1.0 / node_total)
    if step == 0:
        packed, piece_out, state, degree_out, lower_out = outs
        level = total[16:17]
        lower, inverse = factor_and_inverse(gram[:, 0:16])
        block = start[...]
        applied = level * block - total[0:16]
        both = dot_f32(inverse, jnp.concatenate([block, applied], axis=1), ((1,), (0,)))
        degree_out[...] = total[16:24]
        stack = both
        new_vectors = both[:, 0:256]
        new_applied = both[:, 256:512]
        state[...] = both
        basis = new_vectors
        lower_out[...] = lower
    else:
        if step == 1:
            packed, piece_out, state, coeff_out, lower_out, shift_out = outs
        else:
            packed, piece_out, state, coeff_out, lower_out = outs
        width = 16 * step
        coeffs = gram[:, 0:width]
        square = gram[:, width : width + 16]
        square = square - dot_f32(coeffs, coeffs, ((1,), (1,)))
        lower, inverse = factor_and_inverse(square)
        stack = before[...]
        newest = stack[width - 16 : width]
        vectors, applied = newest[:, 0:256], newest[:, 256:512]
        level = degree[0:1]
        twice = level * applied - total[0:16]
        coeff_out[...] = jnp.concatenate([coeffs, jnp.zeros((16, 128 - width), f32)], axis=1)
        if step == 1:
            shift = jnp.broadcast_to(
                jnp.sum(coeffs * eye16(), axis=(0, 1), keepdims=True) * (1.0 / 16), (8, 128)
            )
            shift_out[...] = shift
            scalar = shift[0:1, 0:1]
            moved = applied - scalar * vectors
            twice = twice - scalar * applied - scalar * moved
            coeffs = coeffs - scalar * eye16()
            applied = moved
            stack = jnp.concatenate([vectors, applied], axis=1)
        else:
            scalar = shift_in[0:1, 0:1]
            twice = twice - scalar * applied
            coeff_out[:, width - 16 : width] = coeffs[:, width - 16 : width] + scalar * eye16()
        rest = jnp.concatenate([applied, twice], axis=1) - dot_f32(coeffs, stack, ((1,), (0,)))
        both = dot_f32(inverse, rest, ((1,), (0,)))
        state[0:width] = stack
        state[width : width + 16] = both
        lower_out[...] = lower
        new_applied = both[:, 256:512]
        basis = jnp.concatenate([stack[:, 0:256], both[:, 0:256]], axis=0)
    partial = dot_f32(new_applied, jnp.concatenate([basis, new_applied], axis=0), ((1,), (1,)))
    piece_out[...] = new_applied
    gram_rows = pack_gram(partial)
    if step == ITERS - 1:
        for p in range(packed.shape[0]):
            packed[p] = gram_rows
    else:
        message = jnp.concatenate([new_applied, gram_rows], axis=0)
        for p in range(packed.shape[0]):
            packed[p] = message


def update(step, node_total, arrived, sides, state, degree, shift, start):
    size = arrived.shape[2]
    shapes = [
        jax.ShapeDtypeStruct((8, 8, size) if step == ITERS - 1 else (16, 24, size), f32),
        jax.ShapeDtypeStruct((16, size), f32),
        jax.ShapeDtypeStruct((16 * (step + 1), 2 * size), f32),
    ]
    if step == 0:
        shapes += [jax.ShapeDtypeStruct((8, size), f32), jax.ShapeDtypeStruct((16, 16), f32)]
        extra = [start]
    else:
        shapes += [jax.ShapeDtypeStruct((16, 128), f32), jax.ShapeDtypeStruct((16, 16), f32)]
        extra = [state, degree]
        if step == 1:
            shapes.append(jax.ShapeDtypeStruct((8, 128), f32))
        else:
            extra.append(shift)
    args = [arrived, *sides, *extra]
    return pl.pallas_call(
        functools.partial(update_kernel, step, node_total),
        out_shape=tuple(shapes),
        in_specs=[VMEM] * len(args),
        out_specs=(VMEM,) * len(shapes),
        compiler_params=limits(16),
        cost_estimate=cost(400_000_000),
    )(*args)


def fold_kernel(arrived, packed):
    total = arrived[0]
    for p in range(1, arrived.shape[0]):
        total = total + arrived[p]
    for p in range(packed.shape[0]):
        packed[p] = total


def fold(arrived):
    return pl.pallas_call(
        fold_kernel,
        name="fold",
        out_shape=jax.ShapeDtypeStruct((16, 8, arrived.shape[2]), f32),
        in_specs=[VMEM],
        out_specs=VMEM,
        compiler_params=limits(8),
    )(arrived)


def last_kernel(node_total, arrived, state, shift, *refs):
    coeffs_in, lowers_in = refs[0 : ITERS - 1], refs[ITERS - 1 : 2 * ITERS - 1]
    basis_out, coeffs_out, lowers_out = refs[2 * ITERS - 1 :]
    packed = arrived[0]
    for p in range(1, arrived.shape[0]):
        packed = packed + arrived[p]
    gram = unpack_gram(packed) * (1.0 / node_total)
    width = 16 * ITERS
    coeffs = gram[:, 0:width]
    square = gram[:, width : width + 16] - dot_f32(coeffs, coeffs, ((1,), (1,)))
    stack = state[...]
    rest = stack[width - 16 : width, 256:512] - dot_f32(coeffs, stack[:, 0:256], ((1,), (0,)))
    for k in range(ITERS):
        basis_out[k] = stack[16 * k : 16 * k + 16, 0:256]
        lowers_out[k] = lowers_in[k][...]
        for j in range(ITERS):
            if j > k:
                coeffs_out[k, j] = jnp.zeros((16, 16), f32)
            elif k < ITERS - 1:
                coeffs_out[k, j] = coeffs_in[k][:, 16 * j : 16 * j + 16]
            elif j < k:
                coeffs_out[k, j] = coeffs[:, 16 * j : 16 * j + 16]
            else:
                coeffs_out[k, j] = coeffs[:, 16 * j : 16 * j + 16] + shift[0:1, 0:1] * eye16()
    lower, inverse = factor_and_inverse(square)
    basis_out[ITERS] = dot_f32(inverse, rest, ((1,), (0,)))
    lowers_out[ITERS] = lower


def last(node_total, arrived, state, shift, coeffs, lowers):
    args = [arrived, state, shift, *coeffs, *lowers]
    return pl.pallas_call(
        functools.partial(last_kernel, node_total),
        name="last",
        out_shape=(
            jax.ShapeDtypeStruct((ITERS + 1, 16, arrived.shape[2]), f32),
            jax.ShapeDtypeStruct((ITERS, ITERS, 16, 16), f32),
            jax.ShapeDtypeStruct((ITERS + 1, 16, 16), f32),
        ),
        in_specs=[VMEM] * len(args),
        out_specs=(VMEM,) * 3,
        compiler_params=limits(8),
    )(*args)


def shifted(value, hop):
    size = lax.axis_size("grp")
    return lax.ppermute(value, "grp", [(i, (i + hop) % size) for i in range(size)])


def swapped(value):
    return lax.ppermute(value, CORE, [(0, 1), (1, 0)])


def exchanged(value, axes):
    return lax.all_to_all(value, axes, split_axis=0, concat_axis=0, tiled=True)


def body(start_block, tile_values, tile_row, tile_col, tile_count):
    grp_size = lax.axis_size("grp")
    node_total = float(start_block.shape[1] * grp_size * lax.axis_size(COL))
    message = jnp.broadcast_to(start_block, (lax.axis_size(ZX), *start_block.shape))
    place = tuple(
        pltpu.with_memory_space_constraint(part, pltpu.MemorySpace.HBM)
        for part in (tile_row, tile_col)
    )
    place = (*place, tile_count)
    start_block = pltpu.with_memory_space_constraint(start_block, pltpu.MemorySpace.HBM)
    tile_values = pltpu.with_memory_space_constraint(tile_values, pltpu.MemorySpace.HBM)
    piece = start_block
    state = degree = shift = hi = lo = None
    lowers, coeffs = [], []
    for step in range(ITERS):
        first = step == 0
        pieces = [piece]
        for hop in range(1, grp_size):
            pieces.append(shifted(piece, hop))
        near = exchanged(message, ZX)
        if first:
            rows, hi, lo = rows_first(place, tile_values, pieces)
            hi = pltpu.with_memory_space_constraint(hi, pltpu.MemorySpace.HBM)
            lo = pltpu.with_memory_space_constraint(lo, pltpu.MemorySpace.HBM)
        else:
            rows = rows_next(place, hi, lo, pieces)
        far = swapped(near)
        arrived = exchanged(rows, COL)
        sides = cols_product(first, place, hi, lo, near, far)
        sides = [sides[0]] + [shifted(sides[hop], hop) for hop in range(1, grp_size)]
        outs = update(step, node_total, arrived, sides, state, degree, shift, start_block)
        message, piece, state = outs[0:3]
        if first:
            degree = outs[3]
        else:
            coeffs.append(outs[3])
        lowers.append(outs[4])
        if step == 1:
            shift = outs[5]
    packed = fold(exchanged(message, ("col_1", "col_2")))
    packed = exchanged(packed, ("grp", "col_0"))
    return last(node_total, packed, state, shift, coeffs, lowers)


def solution(mesh):
    split_mesh = Mesh(
        mesh.devices.reshape(mesh.shape["grp"], 4, 4, 2), ("grp", "col_0", "col_1", "col_2")
    )
    placed = (
        P(None, GRP_COL),
        P("grp", COL, None, None, None),
        P("grp", COL, None),
        P("grp", COL, None),
        P("grp", COL),
    )
    return jax.shard_map(
        body,
        mesh=split_mesh,
        in_specs=placed,
        out_specs=(P(None, None, GRP_COL), P(), P()),
        check_vma=False,
    )
```

```python
import functools
import jax
import jax.numpy as jnp
from jax import lax
from jax.experimental import pallas as pl
from jax.experimental.pallas import tpu as pltpu
from jax.sharding import Mesh
from jax.sharding import PartitionSpec as P

ITERS = 4
ZX = ("col_0", "col_1")
CORE = "col_2"
COL = ("col_0", "col_1", "col_2")
GRP_COL = ("grp", "col_0", "col_1", "col_2")
HELD = 4
ROW_GROUP = 8
LATER_ROW_GROUP = 7
COL_GROUP = 4
FACTOR_GROUP = 8
highest = lax.Precision.HIGHEST
VMEM = pl.BlockSpec(memory_space=pltpu.VMEM)
SMEM = pl.BlockSpec(memory_space=pltpu.SMEM)
HBM = pl.BlockSpec(memory_space=pltpu.MemorySpace.HBM)
MIB = 1 << 20
f32 = jnp.float32
bf16 = jnp.bfloat16


def split(x):
    hi = x.astype(bf16)
    return hi, (x - hi.astype(f32)).astype(bf16)


def dot(a, b, dims):
    return lax.dot_general(a, b, (dims, ((), ())), preferred_element_type=f32)


def dot_f32(a, b, dims):
    return lax.dot_general(a, b, (dims, ((), ())), precision=highest, preferred_element_type=f32)


def limits(mib):
    return pltpu.CompilerParams(vmem_limit_bytes=mib * MIB)


def cost(flops):
    return pl.CostEstimate(flops=flops, bytes_accessed=MIB, transcendentals=0)


def products(lhs_hi, lhs_lo, hi, lo, dims, first, live):
    top = dot(lhs_hi, hi, dims)
    low = dot(lhs_lo, lo, dims)
    out = top[0:16] + top[16:32] + low[0:16]
    if first:
        out = jnp.concatenate([out, top[32:40] + low[16:24]], axis=0)
    return jnp.where(live, out, 0.0)


def to_tiles(block):
    halves = [block[8 * r : 8 * r + 8, 128 * c : 128 * c + 128] for r in (0, 1) for c in (0, 1)]
    return jnp.stack(halves)


def from_tiles(tiles):
    rows = [jnp.concatenate([tiles[2 * r], tiles[2 * r + 1]], axis=1) for r in (0, 1)]
    return jnp.concatenate(rows, axis=0)


def with_degree(result):
    sums = result[16:24]
    row = lax.broadcasted_iota(jnp.int32, (8, 128), 0)
    tile = jnp.where(row == 0, sums[:, 0:128], sums[:, 128:256])
    return jnp.concatenate([to_tiles(result[0:16]), tile[None]], axis=0)


def stacked_lhs(piece, first):
    hi, lo = split(piece)
    if first:
        ones = jnp.ones((16, piece.shape[1]), bf16)
        return jnp.concatenate([hi, lo, ones], axis=0), jnp.concatenate([hi, ones], axis=0)
    return jnp.concatenate([hi, lo], axis=0), hi


def fill_pieces(pieces, lhs_hi, lhs_lo, first):
    for k, piece in enumerate(pieces):
        lhs_hi[k], lhs_lo[k] = stacked_lhs(piece[...], first)


def group_rows(base, size, origin, place, lhs_hi, lhs_lo, hi, lo, out, first):
    tile_row, tile_col, tile_count = place
    results = []
    for u in range(size):
        s = base + u
        k = ((tile_row[0, 0, 0] >> 5) - (tile_col[0, 0, s] >> 5)) & 3
        live = s < tile_count[0, 0]
        results.append(
            products(
                lhs_hi[k], lhs_lo[k], hi[s - origin], lo[s - origin], ((1,), (1,)), first, live
            )
        )
    for u in range(size):
        out[tile_row[0, 0, base + u] & 31] += with_degree(results[u]) if first else results[u]


def groups_of(tile_count, group):
    return (tile_count[0, 0] + (group - 1)) // group


def later_groups_of(tile_count, group):
    return (tile_count[0, 0] - HELD + (group - 1)) // group


def part_copies(part, at, source_hi, source_lo, hi, lo, sems):
    return (
        pltpu.make_async_copy(source_hi.at[part], hi.at[part], sems.at[0, at]),
        pltpu.make_async_copy(source_lo.at[part], lo.at[part], sems.at[1, at]),
    )


def group_copies(q, group, *refs):
    return part_copies(pl.ds(q * group, group), q, *refs)


def later_copies(q, group, *refs):
    return part_copies(pl.ds(HELD + q * group, group), q, *refs)


def start_later(tile_count, group, *refs):
    @pl.loop(0, later_groups_of(tile_count, group))
    def _(q):
        for copy in later_copies(q, group, *refs):
            copy.start()


def index_fetch(row_in, col_in, tile_row, tile_col, sems):
    return (
        pltpu.make_async_copy(row_in, tile_row, sems.at[0]),
        pltpu.make_async_copy(col_in, tile_col, sems.at[1]),
    )


def rows_first_kernel(
    row_in, col_in, tile_count, tiles, own, one, two, three, out, hi_held, lo_held, hi_out, lo_out,
    buf, hi, lo, lhs_hi, lhs_lo, tile_row, tile_col, sems, out_sems, index_sems
):
    group = ROW_GROUP
    count = groups_of(tile_count, group)

    def arriving(q):
        part = pl.ds(q * group, group)
        return pltpu.make_async_copy(tiles.at[0, 0, part], buf.at[part], sems.at[q])

    arriving(0).start()
    index_copies = index_fetch(row_in, col_in, tile_row, tile_col, index_sems)
    for copy in index_copies:
        copy.start()

    @pl.loop(1, count)
    def _(q):
        arriving(q).start()

    fill_pieces((own, one, two, three), lhs_hi, lhs_lo, True)
    out[...] = jnp.zeros_like(out)
    for copy in index_copies:
        copy.wait()

    @pl.loop(0, count)
    def _(q):
        arriving(q).wait()
        for u in range(group):
            s = q * group + u
            hi[s], lo[s] = split(buf[s])
        for copy in group_copies(q, group, hi, lo, hi_out, lo_out, out_sems):
            copy.start()
        group_rows(
            q * group, group, 0, (tile_row, tile_col, tile_count), lhs_hi, lhs_lo, hi, lo, out, True
        )

    hi_held[...] = hi[0:HELD]
    lo_held[...] = lo[0:HELD]

    @pl.loop(0, count)
    def _(q):
        for copy in group_copies(q, group, hi, lo, hi_out, lo_out, out_sems):
            copy.wait()


def rows_next_kernel(
    row_in, col_in, tile_count, hi_held, lo_held, hi_in, lo_in, own, one, two, three, out,
    hi, lo, lhs_hi, lhs_lo, tile_row, tile_col, sems, index_sems
):
    group = LATER_ROW_GROUP
    place = (tile_row, tile_col, tile_count)
    index_copies = index_fetch(row_in, col_in, tile_row, tile_col, index_sems)
    for copy in index_copies:
        copy.start()
    start_later(tile_count, group, hi_in, lo_in, hi, lo, sems)
    fill_pieces((own, one, two, three), lhs_hi, lhs_lo, False)
    out[...] = jnp.zeros_like(out)
    for copy in index_copies:
        copy.wait()
    group_rows(0, HELD, 0, place, lhs_hi, lhs_lo, hi_held, lo_held, out, False)

    @pl.loop(0, later_groups_of(tile_count, group))
    def _(q):
        for copy in later_copies(q, group, hi_in, lo_in, hi, lo, sems):
            copy.wait()
        group_rows(HELD + q * group, group, 0, place, lhs_hi, lhs_lo, hi, lo, out, False)


def group_cols(base, size, place, near, far, hi, lo, acc, first):
    tile_row, tile_col, tile_count = place
    results, slots = [], []
    for u in range(size):
        s = base + u
        row = tile_row[0, 0, s] & 31
        at = row >> 1
        same = ((row ^ tile_col[0, 0, 0]) & 1) == 0
        if first:
            piece = jnp.where(same, near[at], far[at])
        else:
            piece = from_tiles(jnp.where(same, near[at, 0:4], far[at, 0:4]))
        left_hi, left_lo = stacked_lhs(piece, first)
        live = s < tile_count[0, 0]
        results.append(products(left_hi, left_lo, hi[s], lo[s], ((1,), (0,)), first, live))
        slots.append(((tile_col[0, 0, s] >> 5) - (tile_row[0, 0, 0] >> 5)) & 3)
    for u in range(size):
        acc[slots[u]] += results[u]


def cols_kernel(
    first, row_in, col_in, tile_count, hi_held, lo_held, hi_in, lo_in, near, far,
    own, one, two, three, hi, lo, acc, tile_row, tile_col, sems, index_sems
):
    group = COL_GROUP
    place = (tile_row, tile_col, tile_count)
    index_copies = index_fetch(row_in, col_in, tile_row, tile_col, index_sems)
    for copy in index_copies:
        copy.start()
    start_later(tile_count, group, hi_in, lo_in, hi, lo, sems)
    acc[...] = jnp.zeros_like(acc)
    for copy in index_copies:
        copy.wait()
    group_cols(0, HELD, place, near, far, hi_held, lo_held, acc, first)
    if first:
        total = jnp.zeros((16, 16), f32)
        for part in (near, far):
            for p in range(part.shape[0]):
                total = total + dot_f32(part[p], part[p], ((1,), (1,)))
        gram = pack_gram(total)
    else:
        gram = jnp.zeros_like(near[0, 4])
        for p in range(near.shape[0]):
            gram = gram + (near[p, 4] + far[p, 4])
    gram = jnp.concatenate([gram, jnp.zeros((8, 128), f32)], axis=1)

    @pl.loop(0, later_groups_of(tile_count, group))
    def _(q):
        for copy in later_copies(q, group, hi_in, lo_in, hi, lo, sems):
            copy.wait()
        group_cols(HELD + q * group, group, place, near, far, hi, lo, acc, first)

    for k, out in enumerate((own, one, two, three)):
        out[...] = jnp.concatenate([acc[k], gram], axis=0)


def rows_first(place, tiles, pieces):
    slots, size = tiles.shape[2], tiles.shape[3]
    return pl.pallas_call(
        rows_first_kernel,
        name="rows_first",
        out_shape=(
            jax.ShapeDtypeStruct((32, 5, 8, 128), f32),
            pltpu.VMEM((HELD, size, size), bf16),
            pltpu.VMEM((HELD, size, size), bf16),
            pltpu.MemorySpace.HBM((slots, size, size), bf16),
            pltpu.MemorySpace.HBM((slots, size, size), bf16),
        ),
        in_specs=[HBM, HBM, SMEM] + [HBM] + [VMEM] * 4,
        out_specs=(VMEM, VMEM, VMEM, HBM, HBM),
        scratch_shapes=[
            pltpu.VMEM((slots, size, size), f32),
            pltpu.VMEM((slots, size, size), bf16),
            pltpu.VMEM((slots, size, size), bf16),
            pltpu.VMEM((4, 48, size), bf16),
            pltpu.VMEM((4, 32, size), bf16),
            pltpu.SMEM((1, 1, slots), jnp.int32),
            pltpu.SMEM((1, 1, slots), jnp.int32),
            pltpu.SemaphoreType.DMA((slots // ROW_GROUP,)),
            pltpu.SemaphoreType.DMA((2, slots // ROW_GROUP)),
            pltpu.SemaphoreType.DMA((2,)),
        ],
        compiler_params=limits(28),
        cost_estimate=cost(400_000_000),
    )(*place, tiles, *pieces)


def rows_next(place, parts, pieces):
    slots, size = parts[2].shape[0], parts[2].shape[1]
    return pl.pallas_call(
        rows_next_kernel,
        name="rows_next",
        out_shape=jax.ShapeDtypeStruct((32, 16, size), f32),
        in_specs=[VMEM, VMEM, SMEM] + [VMEM] * 2 + [HBM] * 2 + [VMEM] * 4,
        out_specs=VMEM,
        scratch_shapes=[
            pltpu.VMEM((slots, size, size), bf16),
            pltpu.VMEM((slots, size, size), bf16),
            pltpu.VMEM((4, 32, size), bf16),
            pltpu.VMEM((4, 16, size), bf16),
            pltpu.SMEM((1, 1, slots), jnp.int32),
            pltpu.SMEM((1, 1, slots), jnp.int32),
            pltpu.SemaphoreType.DMA((2, (slots - HELD) // LATER_ROW_GROUP)),
            pltpu.SemaphoreType.DMA((2,)),
        ],
        compiler_params=limits(20),
        cost_estimate=cost(400_000_000),
    )(*place, *parts, *pieces)


def cols_product(first, place, parts, near, far):
    height = 24 if first else 16
    slots, size = parts[2].shape[0], parts[2].shape[1]
    out = jax.ShapeDtypeStruct((height + 8, size), f32)
    return pl.pallas_call(
        functools.partial(cols_kernel, first),
        name="cols_first" if first else "cols_next",
        out_shape=(out,) * 4,
        in_specs=[VMEM, VMEM, SMEM] + [VMEM] * 2 + [HBM] * 2 + [VMEM] * 2,
        out_specs=(VMEM,) * 4,
        scratch_shapes=[
            pltpu.VMEM((slots, size, size), bf16),
            pltpu.VMEM((slots, size, size), bf16),
            pltpu.VMEM((4, height, size), f32),
            pltpu.SMEM((1, 1, slots), jnp.int32),
            pltpu.SMEM((1, 1, slots), jnp.int32),
            pltpu.SemaphoreType.DMA((2, (slots - HELD) // COL_GROUP)),
            pltpu.SemaphoreType.DMA((2,)),
        ],
        compiler_params=limits(20),
        cost_estimate=cost(400_000_000),
    )(*place, *parts, near, far)


def unpack_gram(packed, width):
    return jnp.concatenate([packed[:, 0:width], packed[:, width : 2 * width]], axis=0)


def pack_gram(gram, width=64):
    if gram.shape[1] < width:
        gram = jnp.concatenate([gram, jnp.zeros((16, width - gram.shape[1]), f32)], axis=1)
    return jnp.concatenate([gram[0:8], gram[8:16]], axis=1)


def eye16():
    return (
        lax.broadcasted_iota(jnp.int32, (16, 16), 0) == lax.broadcasted_iota(jnp.int32, (16, 16), 1)
    ).astype(f32)


def factor_and_inverse(gram):
    work = jnp.concatenate([gram, eye16(), jnp.zeros((16, 96), f32)], axis=1)
    rows = lax.broadcasted_iota(jnp.int32, (16, 128), 0)
    lanes = lax.broadcasted_iota(jnp.int32, (16, 128), 1)
    down = jnp.ones((16, 128), f32)
    across = jnp.ones((16, 128), f32)
    lower = jnp.zeros((16, 128), f32)

    def half(x):
        return jnp.broadcast_to(x, (8, 128))

    def full(x):
        return jnp.concatenate([x, x], axis=0)

    for base in range(0, 16, FACTOR_GROUP):
        group = range(FACTOR_GROUP)
        columns = [jnp.broadcast_to(work[:, base + i : base + i + 1], (16, 128)) for i in group]
        across_rows = [half(work[base + i : base + i + 1]) for i in group]
        corner = {
            (i, k): half(work[base + i : base + i + 1, base + k : base + k + 1])
            for i in group
            for k in range(i + 1)
        }
        scaled = []
        for i in group:
            pivot = corner[i, i]
            inverse = 1.0 / pivot
            for k in range(i + 1, FACTOR_GROUP):
                ratio = corner[k, i] * inverse
                columns[k] = columns[k] - columns[i] * full(ratio)
                across_rows[k] = across_rows[k] - across_rows[i] * ratio
                for m in range(k, FACTOR_GROUP):
                    corner[m, k] = corner[m, k] - ratio * corner[m, i]
            scaled.append(across_rows[i] * inverse)
            at = base + i
            down = jnp.where(rows == at, full(pivot), down)
            across = jnp.where(lanes == at, full(pivot), across)
            lower = jnp.where((lanes == at) & (rows >= at), columns[i], lower)
        for i in group:
            work = work - jnp.where(rows > base + i, columns[i], 0.0) * full(scaled[i])
    lower = lower / jnp.sqrt(across)
    inverse = work / jnp.sqrt(down)
    return lower[:, 0:16], inverse[:, 16:32]


def update_kernel(step, node_total, *refs):
    refs = list(refs)
    take = lambda count: [refs.pop(0) for _ in range(count)]
    (arrived,) = take(1)
    own, one, two, three = take(4)
    before, degree = (None, None) if step == 0 else take(2)
    shift_in = take(1)[0] if step > 1 else None
    (start,) = take(1) if step == 0 else (None,)
    outs = refs
    side = own[...] + one[...] + two[...] + three[...]
    height = side.shape[0] - 8
    total = arrived[0]
    for p in range(1, arrived.shape[0]):
        total = total + arrived[p]
    gram = unpack_gram(side[height : height + 8], 64) * (1.0 / node_total)
    if step == 0:
        level = side[16:17] + jnp.concatenate([total[4, 0:1], total[4, 1:2]], axis=1)
        total = from_tiles(total[0:4])
    total = total + side[0:16]
    if step == 0:
        packed, piece_out, state, degree_out, lower_out = outs
        lower, inverse = factor_and_inverse(gram[:, 0:16])
        block = start[...]
        applied = level * block - total[0:16]
        both = dot_f32(inverse, jnp.concatenate([block, applied], axis=1), ((1,), (0,)))
        degree_out[...] = jnp.broadcast_to(level, degree_out.shape)
        stack = both
        new_vectors = both[:, 0:256]
        new_applied = both[:, 256:512]
        state[...] = both
        basis = new_vectors
        lower_out[...] = lower
    else:
        if step == 1:
            packed, piece_out, state, coeff_out, lower_out, shift_out = outs
        else:
            packed, piece_out, state, coeff_out, lower_out = outs
        width = 16 * step
        coeffs = gram[:, 0:width]
        square = gram[:, width : width + 16]
        square = square - dot_f32(coeffs, coeffs, ((1,), (1,)))
        lower, inverse = factor_and_inverse(square)
        stack = before[...]
        newest = stack[width - 16 : width]
        vectors, applied = newest[:, 0:256], newest[:, 256:512]
        level = degree[0:1]
        twice = level * applied - total[0:16]
        coeff_out[...] = jnp.concatenate([coeffs, jnp.zeros((16, 128 - width), f32)], axis=1)
        if step == 1:
            shift = jnp.broadcast_to(
                jnp.sum(coeffs * eye16(), axis=(0, 1), keepdims=True) * (1.0 / 16), (8, 128)
            )
            shift_out[...] = shift
            scalar = shift[0:1, 0:1]
            moved = applied - scalar * vectors
            twice = twice - scalar * applied - scalar * moved
            coeffs = coeffs - scalar * eye16()
            applied = moved
            stack = jnp.concatenate([vectors, applied], axis=1)
        else:
            scalar = shift_in[0:1, 0:1]
            twice = twice - scalar * applied
            coeff_out[:, width - 16 : width] = coeffs[:, width - 16 : width] + scalar * eye16()
        rest = jnp.concatenate([applied, twice], axis=1) - dot_f32(coeffs, stack, ((1,), (0,)))
        both = dot_f32(inverse, rest, ((1,), (0,)))
        state[0:width] = stack
        state[width : width + 16] = both
        lower_out[...] = lower
        new_applied = both[:, 256:512]
        basis = jnp.concatenate([stack[:, 0:256], both[:, 0:256]], axis=0)
    partial = dot_f32(new_applied, jnp.concatenate([basis, new_applied], axis=0), ((1,), (1,)))
    piece_out[...] = new_applied
    if step == ITERS - 1:
        message = pack_gram(partial, 128)
        for p in range(packed.shape[0]):
            packed[p] = message
    else:
        message = jnp.concatenate([to_tiles(new_applied), pack_gram(partial)[None]], axis=0)
        for p in range(packed.shape[0]):
            packed[p] = message


def update(step, node_total, arrived, sides, state, degree, shift, start):
    size = sides[0].shape[1]
    shapes = [
        jax.ShapeDtypeStruct((8, 8, size) if step == ITERS - 1 else (16, 5, 8, 128), f32),
        jax.ShapeDtypeStruct((16, size), f32),
        jax.ShapeDtypeStruct((16 * (step + 1), 2 * size), f32),
    ]
    if step == 0:
        shapes += [jax.ShapeDtypeStruct((8, size), f32), jax.ShapeDtypeStruct((16, 16), f32)]
        extra = [start]
    else:
        shapes += [jax.ShapeDtypeStruct((16, 128), f32), jax.ShapeDtypeStruct((16, 16), f32)]
        extra = [state, degree]
        if step == 1:
            shapes.append(jax.ShapeDtypeStruct((8, 128), f32))
        else:
            extra.append(shift)
    args = [arrived, *sides, *extra]
    return pl.pallas_call(
        functools.partial(update_kernel, step, node_total),
        out_shape=tuple(shapes),
        in_specs=[VMEM] * len(args),
        out_specs=(VMEM,) * len(shapes),
        compiler_params=limits(16),
        cost_estimate=cost(400_000_000),
    )(*args)


def fold_kernel(arrived, packed):
    total = arrived[0]
    for p in range(1, arrived.shape[0]):
        total = total + arrived[p]
    for p in range(packed.shape[0]):
        packed[p] = total


def fold(arrived):
    return pl.pallas_call(
        fold_kernel,
        name="fold",
        out_shape=jax.ShapeDtypeStruct((16, 8, arrived.shape[2]), f32),
        in_specs=[VMEM],
        out_specs=VMEM,
        compiler_params=limits(8),
    )(arrived)


def last_kernel(node_total, arrived, state, shift, *refs):
    coeffs_in, lowers_in = refs[0 : ITERS - 1], refs[ITERS - 1 : 2 * ITERS - 1]
    basis_out, coeffs_out, lowers_out = refs[2 * ITERS - 1 :]
    packed = arrived[0]
    for p in range(1, arrived.shape[0]):
        packed = packed + arrived[p]
    gram = unpack_gram(packed, 128) * (1.0 / node_total)
    width = 16 * ITERS
    coeffs = gram[:, 0:width]
    square = gram[:, width : width + 16] - dot_f32(coeffs, coeffs, ((1,), (1,)))
    stack = state[...]
    rest = stack[width - 16 : width, 256:512] - dot_f32(coeffs, stack[:, 0:256], ((1,), (0,)))
    for k in range(ITERS):
        basis_out[k] = stack[16 * k : 16 * k + 16, 0:256]
        lowers_out[k] = lowers_in[k][...]
        for j in range(ITERS):
            if j > k:
                coeffs_out[k, j] = jnp.zeros((16, 16), f32)
            elif k < ITERS - 1:
                coeffs_out[k, j] = coeffs_in[k][:, 16 * j : 16 * j + 16]
            elif j < k:
                coeffs_out[k, j] = coeffs[:, 16 * j : 16 * j + 16]
            else:
                coeffs_out[k, j] = coeffs[:, 16 * j : 16 * j + 16] + shift[0:1, 0:1] * eye16()
    lower, inverse = factor_and_inverse(square)
    basis_out[ITERS] = dot_f32(inverse, rest, ((1,), (0,)))
    lowers_out[ITERS] = lower


def last(node_total, arrived, state, shift, coeffs, lowers):
    args = [arrived, state, shift, *coeffs, *lowers]
    return pl.pallas_call(
        functools.partial(last_kernel, node_total),
        name="last",
        out_shape=(
            jax.ShapeDtypeStruct((ITERS + 1, 16, arrived.shape[2]), f32),
            jax.ShapeDtypeStruct((ITERS, ITERS, 16, 16), f32),
            jax.ShapeDtypeStruct((ITERS + 1, 16, 16), f32),
        ),
        in_specs=[VMEM] * len(args),
        out_specs=(VMEM,) * 3,
        compiler_params=limits(8),
    )(*args)


def first_message_kernel(block, packed, piece):
    piece[...] = block[...]
    for p in range(packed.shape[0]):
        packed[p] = block[...]


def first_message(block):
    return pl.pallas_call(
        first_message_kernel,
        name="first_message",
        out_shape=(
            jax.ShapeDtypeStruct((16, *block.shape), f32),
            pltpu.VMEM(block.shape, f32),
        ),
        in_specs=[VMEM],
        out_specs=(VMEM, VMEM),
        compiler_params=limits(4),
    )(block)


def shifted(value, hop):
    size = lax.axis_size("grp")
    return lax.ppermute(value, "grp", [(i, (i + hop) % size) for i in range(size)])


def swapped(value):
    return lax.ppermute(value, CORE, [(0, 1), (1, 0)])


def exchanged(value, axes):
    return lax.all_to_all(value, axes, split_axis=0, concat_axis=0, tiled=True)


def body(start_block, tile_values, tile_row, tile_col, tile_count):
    grp_size = lax.axis_size("grp")
    node_total = float(start_block.shape[1] * grp_size * lax.axis_size(COL))
    HBM_SPACE = pltpu.MemorySpace.HBM

    def placed_in(space):
        index = [pltpu.with_memory_space_constraint(part, space) for part in (tile_row, tile_col)]
        return (*index, tile_count)

    first_place, place = placed_in(HBM_SPACE), placed_in(pltpu.VMEM)
    raw_block = start_block
    start_block = pltpu.with_memory_space_constraint(start_block, HBM_SPACE)
    tile_values = pltpu.with_memory_space_constraint(tile_values, pltpu.MemorySpace.HBM)
    message, piece = first_message(start_block)
    origin = piece
    state = degree = shift = parts = None
    lowers, coeffs = [], []
    for step in range(ITERS):
        first = step == 0
        pieces = [piece]
        for hop in range(1, grp_size):
            pieces.append(shifted(raw_block if first else piece, hop))
        near = exchanged(message, ZX)
        if first:
            rows, *parts = rows_first(first_place, tile_values, pieces)
            parts = [
                pltpu.with_memory_space_constraint(part, space)
                for part, space in zip(
                    parts, (pltpu.VMEM,) * 2 + (pltpu.MemorySpace.HBM,) * 2, strict=True
                )
            ]
        else:
            rows = rows_next(place, parts, pieces)
        far = swapped(near)
        arrived = exchanged(rows, COL)
        cols = cols_product(first, place, parts, near, far)
        sides = [cols[0]]
        for hop in range(1, grp_size):
            sides.append(shifted(cols[hop], hop))
        outs = update(step, node_total, arrived, sides, state, degree, shift, origin)
        message, piece, state = outs[0:3]
        if first:
            degree = outs[3]
        else:
            coeffs.append(outs[3])
        lowers.append(outs[4])
        if step == 1:
            shift = outs[5]
    packed = fold(exchanged(message, ("col_1", "col_2")))
    packed = exchanged(packed, ("grp", "col_0"))
    return last(node_total, packed, state, shift, coeffs, lowers)


def solution(mesh):
    split_mesh = Mesh(
        mesh.devices.reshape(mesh.shape["grp"], 4, 4, 2), ("grp", "col_0", "col_1", "col_2")
    )
    placed = (
        P(None, GRP_COL),
        P("grp", COL, None, None, None),
        P("grp", COL, None),
        P("grp", COL, None),
        P("grp", COL),
    )
    return jax.shard_map(
        body,
        mesh=split_mesh,
        in_specs=placed,
        out_specs=(P(None, None, GRP_COL), P(), P()),
        check_vma=False,
    )
```

```python
import functools
import jax
import jax.numpy as jnp
from jax import lax
from jax.experimental import pallas as pl
from jax.experimental.pallas import tpu as pltpu
from jax.sharding import Mesh
from jax.sharding import PartitionSpec as P

ITERS = 4
ZX = ("col_0", "col_1")
CORE = "col_2"
COL = ("col_0", "col_1", "col_2")
GRP_COL = ("grp", "col_0", "col_1", "col_2")
HELD = 8
ROW_GROUP = HELD
LATER_ROW_GROUP = 8
COL_GROUP = 4
FACTOR_GROUP = 8
highest = lax.Precision.HIGHEST
VMEM = pl.BlockSpec(memory_space=pltpu.VMEM)
SMEM = pl.BlockSpec(memory_space=pltpu.SMEM)
HBM = pl.BlockSpec(memory_space=pltpu.MemorySpace.HBM)
MIB = 1 << 20
f32 = jnp.float32
bf16 = jnp.bfloat16


def split(x):
    hi = x.astype(bf16)
    return hi, (x - hi.astype(f32)).astype(bf16)


def dot(a, b, dims):
    return lax.dot_general(a, b, (dims, ((), ())), preferred_element_type=f32)


def dot_f32(a, b, dims):
    return lax.dot_general(a, b, (dims, ((), ())), precision=highest, preferred_element_type=f32)


def limits(mib):
    return pltpu.CompilerParams(vmem_limit_bytes=mib * MIB)


def cost(flops):
    return pl.CostEstimate(flops=flops, bytes_accessed=MIB, transcendentals=0)


def products(lhs_hi, lhs_lo, hi, lo, dims, first, live):
    top = dot(lhs_hi, hi, dims)
    low = dot(lhs_lo, lo, dims)
    out = top[0:16] + top[16:32] + low[0:16]
    if first:
        out = jnp.concatenate([out, top[32:40] + low[16:24]], axis=0)
    return jnp.where(live, out, 0.0)


def to_tiles(block):
    halves = [block[8 * r : 8 * r + 8, 128 * c : 128 * c + 128] for r in (0, 1) for c in (0, 1)]
    return jnp.stack(halves)


def from_tiles(tiles):
    rows = [jnp.concatenate([tiles[2 * r], tiles[2 * r + 1]], axis=1) for r in (0, 1)]
    return jnp.concatenate(rows, axis=0)


def with_degree(result):
    sums = result[16:24]
    row = lax.broadcasted_iota(jnp.int32, (8, 128), 0)
    tile = jnp.where(row == 0, sums[:, 0:128], sums[:, 128:256])
    return jnp.concatenate([to_tiles(result[0:16]), tile[None]], axis=0)


def stacked_lhs(piece, first):
    hi, lo = split(piece)
    if first:
        ones = jnp.ones((16, piece.shape[1]), bf16)
        return jnp.concatenate([hi, lo, ones], axis=0), jnp.concatenate([hi, ones], axis=0)
    return jnp.concatenate([hi, lo], axis=0), hi


def fill_pieces(pieces, lhs_hi, lhs_lo, first):
    for k, piece in enumerate(pieces):
        lhs_hi[k], lhs_lo[k] = stacked_lhs(piece[...], first)


def group_rows(base, size, origin, place, lhs_hi, lhs_lo, hi, lo, out, first):
    tile_row, tile_col, tile_count = place
    results = []
    for u in range(size):
        s = base + u
        k = ((tile_row[0, 0, 0] >> 5) - (tile_col[0, 0, s] >> 5)) & 3
        live = s < tile_count[0, 0]
        results.append(
            products(
                lhs_hi[k], lhs_lo[k], hi[s - origin], lo[s - origin], ((1,), (1,)), first, live
            )
        )
    for u in range(size):
        out[tile_row[0, 0, base + u] & 31] += with_degree(results[u]) if first else results[u]


def groups_of(tile_count, group):
    return (tile_count[0, 0] + (group - 1)) // group


def later_groups_of(tile_count, group):
    return (tile_count[0, 0] - HELD + (group - 1)) // group


def part_copies(part, at, source_hi, source_lo, hi, lo, sems):
    return (
        pltpu.make_async_copy(source_hi.at[part], hi.at[part], sems.at[0, at]),
        pltpu.make_async_copy(source_lo.at[part], lo.at[part], sems.at[1, at]),
    )


def group_copies(q, group, *refs):
    return part_copies(pl.ds(q * group, group), q, *refs)


def later_copies(q, group, *refs):
    return part_copies(pl.ds(HELD + q * group, group), q, *refs)


def start_later(tile_count, group, *refs):
    @pl.loop(0, later_groups_of(tile_count, group))
    def _(q):
        for copy in later_copies(q, group, *refs):
            copy.start()


def index_fetch(row_in, col_in, tile_row, tile_col, sems):
    return (
        pltpu.make_async_copy(row_in, tile_row, sems.at[0]),
        pltpu.make_async_copy(col_in, tile_col, sems.at[1]),
    )


def rows_first_kernel(
    row_in, col_in, tile_count, tiles, own, one, two, three, out, hi_held, lo_held, hi_out, lo_out,
    buf, hi, lo, lhs_hi, lhs_lo, tile_row, tile_col, sems, out_sems, index_sems
):
    group = ROW_GROUP
    count = groups_of(tile_count, group)

    def arriving(q):
        part = pl.ds(q * group, group)
        return pltpu.make_async_copy(tiles.at[0, 0, part], buf.at[part], sems.at[q])

    arriving(0).start()
    index_copies = index_fetch(row_in, col_in, tile_row, tile_col, index_sems)
    for copy in index_copies:
        copy.start()

    @pl.loop(1, count)
    def _(q):
        arriving(q).start()

    fill_pieces((own, one, two, three), lhs_hi, lhs_lo, True)
    out[...] = jnp.zeros_like(out)
    for copy in index_copies:
        copy.wait()

    place = (tile_row, tile_col, tile_count)
    arriving(0).wait()
    for u in range(HELD):
        hi_held[u], lo_held[u] = split(buf[u])
    group_rows(0, HELD, 0, place, lhs_hi, lhs_lo, hi_held, lo_held, out, True)

    @pl.loop(1, count)
    def _(q):
        arriving(q).wait()
        for u in range(group):
            s = q * group + u
            hi[s], lo[s] = split(buf[s])
        for copy in group_copies(q, group, hi, lo, hi_out, lo_out, out_sems):
            copy.start()
        group_rows(q * group, group, 0, place, lhs_hi, lhs_lo, hi, lo, out, True)

    @pl.loop(1, count)
    def _(q):
        for copy in group_copies(q, group, hi, lo, hi_out, lo_out, out_sems):
            copy.wait()


def rows_next_kernel(
    row_in, col_in, tile_count, hi_held, lo_held, hi_in, lo_in, own, one, two, three, out,
    hi, lo, lhs_hi, lhs_lo, tile_row, tile_col, sems, index_sems
):
    group = LATER_ROW_GROUP
    place = (tile_row, tile_col, tile_count)
    index_copies = index_fetch(row_in, col_in, tile_row, tile_col, index_sems)
    for copy in index_copies:
        copy.start()
    start_later(tile_count, group, hi_in, lo_in, hi, lo, sems)
    fill_pieces((own, one, two, three), lhs_hi, lhs_lo, False)
    out[...] = jnp.zeros_like(out)
    for copy in index_copies:
        copy.wait()
    group_rows(0, HELD, 0, place, lhs_hi, lhs_lo, hi_held, lo_held, out, False)

    @pl.loop(0, later_groups_of(tile_count, group))
    def _(q):
        for copy in later_copies(q, group, hi_in, lo_in, hi, lo, sems):
            copy.wait()
        group_rows(HELD + q * group, group, 0, place, lhs_hi, lhs_lo, hi, lo, out, False)


def group_cols(base, size, place, near, far, hi, lo, acc, first):
    tile_row, tile_col, tile_count = place
    results, slots = [], []
    for u in range(size):
        s = base + u
        row = tile_row[0, 0, s] & 31
        at = row >> 1
        same = ((row ^ tile_col[0, 0, 0]) & 1) == 0
        if first:
            piece = jnp.where(same, near[at], far[at])
        else:
            piece = from_tiles(jnp.where(same, near[at, 0:4], far[at, 0:4]))
        left_hi, left_lo = stacked_lhs(piece, first)
        live = s < tile_count[0, 0]
        results.append(products(left_hi, left_lo, hi[s], lo[s], ((1,), (0,)), first, live))
        slots.append(((tile_col[0, 0, s] >> 5) - (tile_row[0, 0, 0] >> 5)) & 3)
    for u in range(size):
        acc[slots[u]] += results[u]


def cols_kernel(
    first, row_in, col_in, tile_count, hi_held, lo_held, hi_in, lo_in, near, far,
    own, one, two, three, hi, lo, acc, tile_row, tile_col, sems, index_sems
):
    group = COL_GROUP
    place = (tile_row, tile_col, tile_count)
    index_copies = index_fetch(row_in, col_in, tile_row, tile_col, index_sems)
    for copy in index_copies:
        copy.start()
    start_later(tile_count, group, hi_in, lo_in, hi, lo, sems)
    acc[...] = jnp.zeros_like(acc)
    for copy in index_copies:
        copy.wait()
    group_cols(0, HELD, place, near, far, hi_held, lo_held, acc, first)
    if first:
        total = jnp.zeros((16, 16), f32)
        for part in (near, far):
            for p in range(part.shape[0]):
                total = total + dot_f32(part[p], part[p], ((1,), (1,)))
        gram = pack_gram(total)
    else:
        gram = jnp.zeros_like(near[0, 4])
        for p in range(near.shape[0]):
            gram = gram + (near[p, 4] + far[p, 4])
    gram = jnp.concatenate([gram, jnp.zeros((8, 128), f32)], axis=1)

    @pl.loop(0, later_groups_of(tile_count, group))
    def _(q):
        for copy in later_copies(q, group, hi_in, lo_in, hi, lo, sems):
            copy.wait()
        group_cols(HELD + q * group, group, place, near, far, hi, lo, acc, first)

    for k, out in enumerate((own, one, two, three)):
        out[...] = jnp.concatenate([acc[k], gram], axis=0)


def rows_first(place, tiles, pieces):
    slots, size = tiles.shape[2], tiles.shape[3]
    return pl.pallas_call(
        rows_first_kernel,
        name="rows_first",
        out_shape=(
            jax.ShapeDtypeStruct((32, 5, 8, 128), f32),
            pltpu.VMEM((HELD, size, size), bf16),
            pltpu.VMEM((HELD, size, size), bf16),
            pltpu.MemorySpace.HBM((slots, size, size), bf16),
            pltpu.MemorySpace.HBM((slots, size, size), bf16),
        ),
        in_specs=[HBM, HBM, SMEM] + [HBM] + [VMEM] * 4,
        out_specs=(VMEM, VMEM, VMEM, HBM, HBM),
        scratch_shapes=[
            pltpu.VMEM((slots, size, size), f32),
            pltpu.VMEM((slots, size, size), bf16),
            pltpu.VMEM((slots, size, size), bf16),
            pltpu.VMEM((4, 48, size), bf16),
            pltpu.VMEM((4, 32, size), bf16),
            pltpu.SMEM((1, 1, slots), jnp.int32),
            pltpu.SMEM((1, 1, slots), jnp.int32),
            pltpu.SemaphoreType.DMA((slots // ROW_GROUP,)),
            pltpu.SemaphoreType.DMA((2, slots // ROW_GROUP)),
            pltpu.SemaphoreType.DMA((2,)),
        ],
        compiler_params=limits(28),
        cost_estimate=cost(400_000_000),
    )(*place, tiles, *pieces)


def rows_next(place, parts, pieces):
    slots, size = parts[2].shape[0], parts[2].shape[1]
    return pl.pallas_call(
        rows_next_kernel,
        name="rows_next",
        out_shape=jax.ShapeDtypeStruct((32, 16, size), f32),
        in_specs=[VMEM, VMEM, SMEM] + [VMEM] * 2 + [HBM] * 2 + [VMEM] * 4,
        out_specs=VMEM,
        scratch_shapes=[
            pltpu.VMEM((slots, size, size), bf16),
            pltpu.VMEM((slots, size, size), bf16),
            pltpu.VMEM((4, 32, size), bf16),
            pltpu.VMEM((4, 16, size), bf16),
            pltpu.SMEM((1, 1, slots), jnp.int32),
            pltpu.SMEM((1, 1, slots), jnp.int32),
            pltpu.SemaphoreType.DMA((2, (slots - HELD) // LATER_ROW_GROUP)),
            pltpu.SemaphoreType.DMA((2,)),
        ],
        compiler_params=limits(20),
        cost_estimate=cost(400_000_000),
    )(*place, *parts, *pieces)


def cols_product(first, place, parts, near, far):
    height = 24 if first else 16
    slots, size = parts[2].shape[0], parts[2].shape[1]
    out = jax.ShapeDtypeStruct((height + 8, size), f32)
    return pl.pallas_call(
        functools.partial(cols_kernel, first),
        name="cols_first" if first else "cols_next",
        out_shape=(out,) * 4,
        in_specs=[VMEM, VMEM, SMEM] + [VMEM] * 2 + [HBM] * 2 + [VMEM] * 2,
        out_specs=(VMEM,) * 4,
        scratch_shapes=[
            pltpu.VMEM((slots, size, size), bf16),
            pltpu.VMEM((slots, size, size), bf16),
            pltpu.VMEM((4, height, size), f32),
            pltpu.SMEM((1, 1, slots), jnp.int32),
            pltpu.SMEM((1, 1, slots), jnp.int32),
            pltpu.SemaphoreType.DMA((2, (slots - HELD) // COL_GROUP)),
            pltpu.SemaphoreType.DMA((2,)),
        ],
        compiler_params=limits(20),
        cost_estimate=cost(400_000_000),
    )(*place, *parts, near, far)


def unpack_gram(packed, width):
    return jnp.concatenate([packed[:, 0:width], packed[:, width : 2 * width]], axis=0)


def pack_gram(gram, width=64):
    if gram.shape[1] < width:
        gram = jnp.concatenate([gram, jnp.zeros((16, width - gram.shape[1]), f32)], axis=1)
    return jnp.concatenate([gram[0:8], gram[8:16]], axis=1)


def eye16():
    return (
        lax.broadcasted_iota(jnp.int32, (16, 16), 0) == lax.broadcasted_iota(jnp.int32, (16, 16), 1)
    ).astype(f32)


def factor_and_inverse(gram):
    work = jnp.concatenate([gram, eye16(), jnp.zeros((16, 96), f32)], axis=1)
    rows = lax.broadcasted_iota(jnp.int32, (16, 128), 0)
    lanes = lax.broadcasted_iota(jnp.int32, (16, 128), 1)
    down = jnp.ones((16, 128), f32)
    across = jnp.ones((16, 128), f32)
    lower = jnp.zeros((16, 128), f32)

    def half(x):
        return jnp.broadcast_to(x, (8, 128))

    def full(x):
        return jnp.concatenate([x, x], axis=0)

    for base in range(0, 16, FACTOR_GROUP):
        group = range(FACTOR_GROUP)
        columns = [jnp.broadcast_to(work[:, base + i : base + i + 1], (16, 128)) for i in group]
        across_rows = [half(work[base + i : base + i + 1]) for i in group]
        corner = {
            (i, k): half(work[base + i : base + i + 1, base + k : base + k + 1])
            for i in group
            for k in range(i + 1)
        }
        scaled = []
        for i in group:
            pivot = corner[i, i]
            inverse = 1.0 / pivot
            for k in range(i + 1, FACTOR_GROUP):
                ratio = corner[k, i] * inverse
                columns[k] = columns[k] - columns[i] * full(ratio)
                across_rows[k] = across_rows[k] - across_rows[i] * ratio
                for m in range(k, FACTOR_GROUP):
                    corner[m, k] = corner[m, k] - ratio * corner[m, i]
            scaled.append(across_rows[i] * inverse)
            at = base + i
            down = jnp.where(rows == at, full(pivot), down)
            across = jnp.where(lanes == at, full(pivot), across)
            lower = jnp.where((lanes == at) & (rows >= at), columns[i], lower)
        for i in group:
            work = work - jnp.where(rows > base + i, columns[i], 0.0) * full(scaled[i])
    lower = lower / jnp.sqrt(across)
    inverse = work / jnp.sqrt(down)
    return lower[:, 0:16], inverse[:, 16:32]


def update_kernel(step, node_total, *refs):
    refs = list(refs)
    take = lambda count: [refs.pop(0) for _ in range(count)]
    (arrived,) = take(1)
    own, one, two, three = take(4)
    before, degree = (None, None) if step == 0 else take(2)
    shift_in = take(1)[0] if step > 1 else None
    (start,) = take(1) if step == 0 else (None,)
    outs = refs
    side = own[...] + one[...] + two[...] + three[...]
    height = side.shape[0] - 8
    total = arrived[0]
    for p in range(1, arrived.shape[0]):
        total = total + arrived[p]
    gram = unpack_gram(side[height : height + 8], 64) * (1.0 / node_total)
    if step == 0:
        level = side[16:17] + jnp.concatenate([total[4, 0:1], total[4, 1:2]], axis=1)
        total = from_tiles(total[0:4])
    total = total + side[0:16]
    if step == 0:
        packed, piece_out, state, degree_out, lower_out = outs
        lower, inverse = factor_and_inverse(gram[:, 0:16])
        block = start[...]
        applied = level * block - total[0:16]
        both = dot_f32(inverse, jnp.concatenate([block, applied], axis=1), ((1,), (0,)))
        degree_out[...] = jnp.broadcast_to(level, degree_out.shape)
        stack = both
        new_vectors = both[:, 0:256]
        new_applied = both[:, 256:512]
        state[...] = both
        basis = new_vectors
        lower_out[...] = lower
    else:
        if step == 1:
            packed, piece_out, state, coeff_out, lower_out, shift_out = outs
        else:
            packed, piece_out, state, coeff_out, lower_out = outs
        width = 16 * step
        coeffs = gram[:, 0:width]
        square = gram[:, width : width + 16]
        square = square - dot_f32(coeffs, coeffs, ((1,), (1,)))
        lower, inverse = factor_and_inverse(square)
        stack = before[...]
        newest = stack[width - 16 : width]
        vectors, applied = newest[:, 0:256], newest[:, 256:512]
        level = degree[0:1]
        twice = level * applied - total[0:16]
        coeff_out[...] = jnp.concatenate([coeffs, jnp.zeros((16, 128 - width), f32)], axis=1)
        if step == 1:
            shift = jnp.broadcast_to(
                jnp.sum(coeffs * eye16(), axis=(0, 1), keepdims=True) * (1.0 / 16), (8, 128)
            )
            shift_out[...] = shift
            scalar = shift[0:1, 0:1]
            moved = applied - scalar * vectors
            twice = twice - scalar * applied - scalar * moved
            coeffs = coeffs - scalar * eye16()
            applied = moved
            stack = jnp.concatenate([vectors, applied], axis=1)
        else:
            scalar = shift_in[0:1, 0:1]
            twice = twice - scalar * applied
            coeff_out[:, width - 16 : width] = coeffs[:, width - 16 : width] + scalar * eye16()
        rest = jnp.concatenate([applied, twice], axis=1) - dot_f32(coeffs, stack, ((1,), (0,)))
        both = dot_f32(inverse, rest, ((1,), (0,)))
        state[0:width] = stack
        state[width : width + 16] = both
        lower_out[...] = lower
        new_applied = both[:, 256:512]
        basis = jnp.concatenate([stack[:, 0:256], both[:, 0:256]], axis=0)
    partial = dot_f32(new_applied, jnp.concatenate([basis, new_applied], axis=0), ((1,), (1,)))
    piece_out[...] = new_applied
    if step == ITERS - 1:
        message = pack_gram(partial, 128)
        for p in range(packed.shape[0]):
            packed[p] = message
    else:
        message = jnp.concatenate([to_tiles(new_applied), pack_gram(partial)[None]], axis=0)
        for p in range(packed.shape[0]):
            packed[p] = message


def update(step, node_total, arrived, sides, state, degree, shift, start):
    size = sides[0].shape[1]
    shapes = [
        jax.ShapeDtypeStruct((8, 8, size) if step == ITERS - 1 else (16, 5, 8, 128), f32),
        jax.ShapeDtypeStruct((16, size), f32),
        jax.ShapeDtypeStruct((16 * (step + 1), 2 * size), f32),
    ]
    if step == 0:
        shapes += [jax.ShapeDtypeStruct((8, size), f32), jax.ShapeDtypeStruct((16, 16), f32)]
        extra = [start]
    else:
        shapes += [jax.ShapeDtypeStruct((16, 128), f32), jax.ShapeDtypeStruct((16, 16), f32)]
        extra = [state, degree]
        if step == 1:
            shapes.append(jax.ShapeDtypeStruct((8, 128), f32))
        else:
            extra.append(shift)
    args = [arrived, *sides, *extra]
    return pl.pallas_call(
        functools.partial(update_kernel, step, node_total),
        out_shape=tuple(shapes),
        in_specs=[VMEM] * len(args),
        out_specs=(VMEM,) * len(shapes),
        compiler_params=limits(16),
        cost_estimate=cost(400_000_000),
    )(*args)


def fold_kernel(arrived, packed):
    total = arrived[0]
    for p in range(1, arrived.shape[0]):
        total = total + arrived[p]
    for p in range(packed.shape[0]):
        packed[p] = total


def fold(arrived):
    return pl.pallas_call(
        fold_kernel,
        name="fold",
        out_shape=jax.ShapeDtypeStruct((16, 8, arrived.shape[2]), f32),
        in_specs=[VMEM],
        out_specs=VMEM,
        compiler_params=limits(8),
    )(arrived)


def last_kernel(node_total, arrived, state, shift, *refs):
    coeffs_in, lowers_in = refs[0 : ITERS - 1], refs[ITERS - 1 : 2 * ITERS - 1]
    basis_out, coeffs_out, lowers_out = refs[2 * ITERS - 1 :]
    packed = arrived[0]
    for p in range(1, arrived.shape[0]):
        packed = packed + arrived[p]
    gram = unpack_gram(packed, 128) * (1.0 / node_total)
    width = 16 * ITERS
    coeffs = gram[:, 0:width]
    square = gram[:, width : width + 16] - dot_f32(coeffs, coeffs, ((1,), (1,)))
    stack = state[...]
    rest = stack[width - 16 : width, 256:512] - dot_f32(coeffs, stack[:, 0:256], ((1,), (0,)))
    for k in range(ITERS):
        basis_out[k] = stack[16 * k : 16 * k + 16, 0:256]
        lowers_out[k] = lowers_in[k][...]
        for j in range(ITERS):
            if j > k:
                coeffs_out[k, j] = jnp.zeros((16, 16), f32)
            elif k < ITERS - 1:
                coeffs_out[k, j] = coeffs_in[k][:, 16 * j : 16 * j + 16]
            elif j < k:
                coeffs_out[k, j] = coeffs[:, 16 * j : 16 * j + 16]
            else:
                coeffs_out[k, j] = coeffs[:, 16 * j : 16 * j + 16] + shift[0:1, 0:1] * eye16()
    lower, inverse = factor_and_inverse(square)
    basis_out[ITERS] = dot_f32(inverse, rest, ((1,), (0,)))
    lowers_out[ITERS] = lower


def last(node_total, arrived, state, shift, coeffs, lowers):
    args = [arrived, state, shift, *coeffs, *lowers]
    return pl.pallas_call(
        functools.partial(last_kernel, node_total),
        name="last",
        out_shape=(
            jax.ShapeDtypeStruct((ITERS + 1, 16, arrived.shape[2]), f32),
            jax.ShapeDtypeStruct((ITERS, ITERS, 16, 16), f32),
            jax.ShapeDtypeStruct((ITERS + 1, 16, 16), f32),
        ),
        in_specs=[VMEM] * len(args),
        out_specs=(VMEM,) * 3,
        compiler_params=limits(8),
    )(*args)


def first_message_kernel(block, packed, piece):
    piece[...] = block[...]
    for p in range(packed.shape[0]):
        packed[p] = block[...]


def first_message(block):
    return pl.pallas_call(
        first_message_kernel,
        name="first_message",
        out_shape=(
            jax.ShapeDtypeStruct((16, *block.shape), f32),
            pltpu.VMEM(block.shape, f32),
        ),
        in_specs=[VMEM],
        out_specs=(VMEM, VMEM),
        compiler_params=limits(4),
    )(block)


def shifted(value, hop):
    size = lax.axis_size("grp")
    return lax.ppermute(value, "grp", [(i, (i + hop) % size) for i in range(size)])


def swapped(value):
    return lax.ppermute(value, CORE, [(0, 1), (1, 0)])


def exchanged(value, axes):
    return lax.all_to_all(value, axes, split_axis=0, concat_axis=0, tiled=True)


def body(start_block, tile_values, tile_row, tile_col, tile_count):
    grp_size = lax.axis_size("grp")
    node_total = float(start_block.shape[1] * grp_size * lax.axis_size(COL))
    HBM_SPACE = pltpu.MemorySpace.HBM

    def placed_in(space):
        index = [pltpu.with_memory_space_constraint(part, space) for part in (tile_row, tile_col)]
        return (*index, tile_count)

    first_place, place = placed_in(HBM_SPACE), placed_in(pltpu.VMEM)
    raw_block = start_block
    start_block = pltpu.with_memory_space_constraint(start_block, HBM_SPACE)
    tile_values = pltpu.with_memory_space_constraint(tile_values, pltpu.MemorySpace.HBM)
    message, piece = first_message(start_block)
    origin = piece
    state = degree = shift = parts = None
    lowers, coeffs = [], []
    for step in range(ITERS):
        first = step == 0
        pieces = [piece]
        for hop in range(1, grp_size):
            pieces.append(shifted(raw_block if first else piece, hop))
        near = exchanged(message, ZX)
        if first:
            rows, *parts = rows_first(first_place, tile_values, pieces)
            parts = [
                pltpu.with_memory_space_constraint(part, space)
                for part, space in zip(
                    parts, (pltpu.VMEM,) * 2 + (pltpu.MemorySpace.HBM,) * 2, strict=True
                )
            ]
        else:
            rows = rows_next(place, parts, pieces)
        far = swapped(near)
        arrived = exchanged(rows, COL)
        cols = cols_product(first, place, parts, near, far)
        sides = [cols[0]]
        for hop in range(1, grp_size):
            sides.append(shifted(cols[hop], hop))
        outs = update(step, node_total, arrived, sides, state, degree, shift, origin)
        message, piece, state = outs[0:3]
        if first:
            degree = outs[3]
        else:
            coeffs.append(outs[3])
        lowers.append(outs[4])
        if step == 1:
            shift = outs[5]
    packed = fold(exchanged(message, ("col_1", "col_2")))
    packed = exchanged(packed, ("grp", "col_0"))
    return last(node_total, packed, state, shift, coeffs, lowers)


def solution(mesh):
    split_mesh = Mesh(
        mesh.devices.reshape(mesh.shape["grp"], 4, 4, 2), ("grp", "col_0", "col_1", "col_2")
    )
    placed = (
        P(None, GRP_COL),
        P("grp", COL, None, None, None),
        P("grp", COL, None),
        P("grp", COL, None),
        P("grp", COL),
    )
    return jax.shard_map(
        body,
        mesh=split_mesh,
        in_specs=placed,
        out_specs=(P(None, None, GRP_COL), P(), P()),
        check_vma=False,
    )
```

```python
import functools
import jax
import jax.numpy as jnp
from jax import lax
from jax.experimental import pallas as pl
from jax.experimental.pallas import tpu as pltpu
from jax.sharding import Mesh
from jax.sharding import PartitionSpec as P

ITERS = 4
ZX = ("col_0", "col_1")
CORE = "col_2"
COL = ("col_0", "col_1", "col_2")
GRP_COL = ("grp", "col_0", "col_1", "col_2")
HELD = 8
AHEAD = 4
ROW_GROUP = HELD
LATER_ROW_GROUP = 8
COL_GROUP = 4
FACTOR_GROUP = 8
highest = lax.Precision.HIGHEST
VMEM = pl.BlockSpec(memory_space=pltpu.VMEM)
SMEM = pl.BlockSpec(memory_space=pltpu.SMEM)
HBM = pl.BlockSpec(memory_space=pltpu.MemorySpace.HBM)
MIB = 1 << 20
f32 = jnp.float32
bf16 = jnp.bfloat16


def split(x):
    hi = x.astype(bf16)
    return hi, (x - hi.astype(f32)).astype(bf16)


def dot(a, b, dims):
    return lax.dot_general(a, b, (dims, ((), ())), preferred_element_type=f32)


def dot_f32(a, b, dims):
    return lax.dot_general(a, b, (dims, ((), ())), precision=highest, preferred_element_type=f32)


def limits(mib):
    return pltpu.CompilerParams(vmem_limit_bytes=mib * MIB)


def cost(flops):
    return pl.CostEstimate(flops=flops, bytes_accessed=MIB, transcendentals=0)


def products(lhs_hi, lhs_lo, hi, lo, dims, first, live):
    top = dot(lhs_hi, hi, dims)
    low = dot(lhs_lo, lo, dims)
    out = top[0:16] + top[16:32] + low[0:16]
    if first:
        out = jnp.concatenate([out, top[32:40] + low[16:24]], axis=0)
    return jnp.where(live, out, 0.0)


def to_tiles(block):
    halves = [block[8 * r : 8 * r + 8, 128 * c : 128 * c + 128] for r in (0, 1) for c in (0, 1)]
    return jnp.stack(halves)


def from_tiles(tiles):
    rows = [jnp.concatenate([tiles[2 * r], tiles[2 * r + 1]], axis=1) for r in (0, 1)]
    return jnp.concatenate(rows, axis=0)


def with_degree(result):
    sums = result[16:24]
    row = lax.broadcasted_iota(jnp.int32, (8, 128), 0)
    tile = jnp.where(row == 0, sums[:, 0:128], sums[:, 128:256])
    return jnp.concatenate([to_tiles(result[0:16]), tile[None]], axis=0)


def stacked_lhs(piece, first):
    hi, lo = split(piece)
    if first:
        ones = jnp.ones((16, piece.shape[1]), bf16)
        return jnp.concatenate([hi, lo, ones], axis=0), jnp.concatenate([hi, ones], axis=0)
    return jnp.concatenate([hi, lo], axis=0), hi


def fill_pieces(pieces, lhs_hi, lhs_lo, first):
    for k, piece in enumerate(pieces):
        lhs_hi[k], lhs_lo[k] = stacked_lhs(piece[...], first)


def group_rows(base, size, origin, place, lhs_hi, lhs_lo, hi, lo, out, first):
    tile_row, tile_col, tile_count = place
    results = []
    for u in range(size):
        s = base + u
        k = ((tile_row[0, 0, 0] >> 5) - (tile_col[0, 0, s] >> 5)) & 3
        live = s < tile_count[0, 0]
        results.append(
            products(
                lhs_hi[k], lhs_lo[k], hi[s - origin], lo[s - origin], ((1,), (1,)), first, live
            )
        )
    for u in range(size):
        out[tile_row[0, 0, base + u] & 31] += with_degree(results[u]) if first else results[u]


def groups_of(tile_count, group):
    return (tile_count[0, 0] + (group - 1)) // group


def later_groups_of(tile_count, group):
    return (tile_count[0, 0] - HELD + (group - 1)) // group


def part_copies(part, at, source_hi, source_lo, hi, lo, sems):
    return (
        pltpu.make_async_copy(source_hi.at[part], hi.at[part], sems.at[0, at]),
        pltpu.make_async_copy(source_lo.at[part], lo.at[part], sems.at[1, at]),
    )


def group_copies(q, group, *refs):
    return part_copies(pl.ds(q * group, group), q, *refs)


def later_copies(q, group, *refs):
    return part_copies(pl.ds(HELD + q * group, group), q, *refs)


def start_later(tile_count, group, *refs):
    @pl.loop(0, later_groups_of(tile_count, group))
    def _(q):
        for copy in later_copies(q, group, *refs):
            copy.start()


def index_fetch(row_in, col_in, tile_row, tile_col, sems):
    return (
        pltpu.make_async_copy(row_in, tile_row, sems.at[0]),
        pltpu.make_async_copy(col_in, tile_col, sems.at[1]),
    )


def rows_first_kernel(
    row_in, col_in, tile_count, tiles, ahead, own, one, two, three, out, hi_held, lo_held, hi_out, lo_out,
    buf, hi, lo, lhs_hi, lhs_lo, tile_row, tile_col, sems, out_sems, index_sems
):
    group = ROW_GROUP
    count = groups_of(tile_count, group)

    def arriving(q):
        part = pl.ds(q * group, group)
        return pltpu.make_async_copy(tiles.at[0, 0, part], buf.at[part], sems.at[q])

    rest = pl.ds(AHEAD, HELD - AHEAD)
    rest_copy = pltpu.make_async_copy(tiles.at[0, 0, rest], buf.at[rest], sems.at[0])
    rest_copy.start()
    index_copies = index_fetch(row_in, col_in, tile_row, tile_col, index_sems)
    for copy in index_copies:
        copy.start()

    @pl.loop(1, count)
    def _(q):
        arriving(q).start()

    fill_pieces((own, one, two, three), lhs_hi, lhs_lo, True)
    out[...] = jnp.zeros_like(out)
    for copy in index_copies:
        copy.wait()

    place = (tile_row, tile_col, tile_count)
    for u in range(AHEAD):
        hi_held[u], lo_held[u] = split(ahead[u])
    group_rows(0, AHEAD, 0, place, lhs_hi, lhs_lo, hi_held, lo_held, out, True)
    rest_copy.wait()
    for u in range(AHEAD, HELD):
        hi_held[u], lo_held[u] = split(buf[u])
    group_rows(AHEAD, HELD - AHEAD, 0, place, lhs_hi, lhs_lo, hi_held, lo_held, out, True)

    @pl.loop(1, count)
    def _(q):
        arriving(q).wait()
        for u in range(group):
            s = q * group + u
            hi[s], lo[s] = split(buf[s])
        for copy in group_copies(q, group, hi, lo, hi_out, lo_out, out_sems):
            copy.start()
        group_rows(q * group, group, 0, place, lhs_hi, lhs_lo, hi, lo, out, True)

    @pl.loop(1, count)
    def _(q):
        for copy in group_copies(q, group, hi, lo, hi_out, lo_out, out_sems):
            copy.wait()


def rows_next_kernel(
    row_in, col_in, tile_count, hi_held, lo_held, hi_in, lo_in, own, one, two, three, out,
    hi, lo, lhs_hi, lhs_lo, tile_row, tile_col, sems, index_sems
):
    group = LATER_ROW_GROUP
    place = (tile_row, tile_col, tile_count)
    index_copies = index_fetch(row_in, col_in, tile_row, tile_col, index_sems)
    for copy in index_copies:
        copy.start()
    start_later(tile_count, group, hi_in, lo_in, hi, lo, sems)
    fill_pieces((own, one, two, three), lhs_hi, lhs_lo, False)
    out[...] = jnp.zeros_like(out)
    for copy in index_copies:
        copy.wait()
    group_rows(0, HELD, 0, place, lhs_hi, lhs_lo, hi_held, lo_held, out, False)

    @pl.loop(0, later_groups_of(tile_count, group))
    def _(q):
        for copy in later_copies(q, group, hi_in, lo_in, hi, lo, sems):
            copy.wait()
        group_rows(HELD + q * group, group, 0, place, lhs_hi, lhs_lo, hi, lo, out, False)


def group_cols(base, size, place, near, far, hi, lo, acc, first):
    tile_row, tile_col, tile_count = place
    results, slots = [], []
    for u in range(size):
        s = base + u
        row = tile_row[0, 0, s] & 31
        at = row >> 1
        same = ((row ^ tile_col[0, 0, 0]) & 1) == 0
        if first:
            piece = jnp.where(same, near[at], far[at])
        else:
            piece = from_tiles(jnp.where(same, near[at, 0:4], far[at, 0:4]))
        left_hi, left_lo = stacked_lhs(piece, first)
        live = s < tile_count[0, 0]
        results.append(products(left_hi, left_lo, hi[s], lo[s], ((1,), (0,)), first, live))
        slots.append(((tile_col[0, 0, s] >> 5) - (tile_row[0, 0, 0] >> 5)) & 3)
    for u in range(size):
        acc[slots[u]] += results[u]


def cols_kernel(
    first, row_in, col_in, tile_count, hi_held, lo_held, hi_in, lo_in, near, far,
    own, one, two, three, hi, lo, acc, tile_row, tile_col, sems, index_sems
):
    group = COL_GROUP
    place = (tile_row, tile_col, tile_count)
    index_copies = index_fetch(row_in, col_in, tile_row, tile_col, index_sems)
    for copy in index_copies:
        copy.start()
    start_later(tile_count, group, hi_in, lo_in, hi, lo, sems)
    acc[...] = jnp.zeros_like(acc)
    for copy in index_copies:
        copy.wait()
    group_cols(0, HELD, place, near, far, hi_held, lo_held, acc, first)
    if first:
        total = jnp.zeros((16, 16), f32)
        for part in (near, far):
            for p in range(part.shape[0]):
                total = total + dot_f32(part[p], part[p], ((1,), (1,)))
        gram = pack_gram(total)
    else:
        gram = jnp.zeros_like(near[0, 4])
        for p in range(near.shape[0]):
            gram = gram + (near[p, 4] + far[p, 4])
    gram = jnp.concatenate([gram, jnp.zeros((8, 128), f32)], axis=1)

    @pl.loop(0, later_groups_of(tile_count, group))
    def _(q):
        for copy in later_copies(q, group, hi_in, lo_in, hi, lo, sems):
            copy.wait()
        group_cols(HELD + q * group, group, place, near, far, hi, lo, acc, first)

    for k, out in enumerate((own, one, two, three)):
        out[...] = jnp.concatenate([acc[k], gram], axis=0)


def rows_first(place, tiles, ahead, pieces):
    slots, size = tiles.shape[2], tiles.shape[3]
    return pl.pallas_call(
        rows_first_kernel,
        name="rows_first",
        out_shape=(
            pltpu.MemorySpace.HBM((32, 5, 8, 128), f32),
            pltpu.VMEM((HELD, size, size), bf16),
            pltpu.VMEM((HELD, size, size), bf16),
            pltpu.MemorySpace.HBM((slots, size, size), bf16),
            pltpu.MemorySpace.HBM((slots, size, size), bf16),
        ),
        in_specs=[HBM, HBM, SMEM] + [HBM] + [VMEM] * 5,
        out_specs=(VMEM, VMEM, VMEM, HBM, HBM),
        scratch_shapes=[
            pltpu.VMEM((slots, size, size), f32),
            pltpu.VMEM((slots, size, size), bf16),
            pltpu.VMEM((slots, size, size), bf16),
            pltpu.VMEM((4, 48, size), bf16),
            pltpu.VMEM((4, 32, size), bf16),
            pltpu.SMEM((1, 1, slots), jnp.int32),
            pltpu.SMEM((1, 1, slots), jnp.int32),
            pltpu.SemaphoreType.DMA((slots // ROW_GROUP,)),
            pltpu.SemaphoreType.DMA((2, slots // ROW_GROUP)),
            pltpu.SemaphoreType.DMA((2,)),
        ],
        compiler_params=limits(28),
        cost_estimate=cost(400_000_000),
    )(*place, tiles, ahead, *pieces)


def rows_next(place, parts, pieces):
    slots, size = parts[2].shape[0], parts[2].shape[1]
    return pl.pallas_call(
        rows_next_kernel,
        name="rows_next",
        out_shape=jax.ShapeDtypeStruct((32, 16, size), f32),
        in_specs=[VMEM, VMEM, SMEM] + [VMEM] * 2 + [HBM] * 2 + [VMEM] * 4,
        out_specs=VMEM,
        scratch_shapes=[
            pltpu.VMEM((slots, size, size), bf16),
            pltpu.VMEM((slots, size, size), bf16),
            pltpu.VMEM((4, 32, size), bf16),
            pltpu.VMEM((4, 16, size), bf16),
            pltpu.SMEM((1, 1, slots), jnp.int32),
            pltpu.SMEM((1, 1, slots), jnp.int32),
            pltpu.SemaphoreType.DMA((2, (slots - HELD) // LATER_ROW_GROUP)),
            pltpu.SemaphoreType.DMA((2,)),
        ],
        compiler_params=limits(20),
        cost_estimate=cost(400_000_000),
    )(*place, *parts, *pieces)


def cols_product(first, place, parts, near, far):
    height = 24 if first else 16
    slots, size = parts[2].shape[0], parts[2].shape[1]
    out = jax.ShapeDtypeStruct((height + 8, size), f32)
    return pl.pallas_call(
        functools.partial(cols_kernel, first),
        name="cols_first" if first else "cols_next",
        out_shape=(out,) * 4,
        in_specs=[VMEM, VMEM, SMEM] + [VMEM] * 2 + [HBM] * 2 + [VMEM] * 2,
        out_specs=(VMEM,) * 4,
        scratch_shapes=[
            pltpu.VMEM((slots, size, size), bf16),
            pltpu.VMEM((slots, size, size), bf16),
            pltpu.VMEM((4, height, size), f32),
            pltpu.SMEM((1, 1, slots), jnp.int32),
            pltpu.SMEM((1, 1, slots), jnp.int32),
            pltpu.SemaphoreType.DMA((2, (slots - HELD) // COL_GROUP)),
            pltpu.SemaphoreType.DMA((2,)),
        ],
        compiler_params=limits(20),
        cost_estimate=cost(400_000_000),
    )(*place, *parts, near, far)


def unpack_gram(packed, width):
    return jnp.concatenate([packed[:, 0:width], packed[:, width : 2 * width]], axis=0)


def pack_gram(gram, width=64):
    if gram.shape[1] < width:
        gram = jnp.concatenate([gram, jnp.zeros((16, width - gram.shape[1]), f32)], axis=1)
    return jnp.concatenate([gram[0:8], gram[8:16]], axis=1)


def eye16():
    return (
        lax.broadcasted_iota(jnp.int32, (16, 16), 0) == lax.broadcasted_iota(jnp.int32, (16, 16), 1)
    ).astype(f32)


def factor_and_inverse(gram):
    work = jnp.concatenate([gram, eye16(), jnp.zeros((16, 96), f32)], axis=1)
    rows = lax.broadcasted_iota(jnp.int32, (16, 128), 0)
    lanes = lax.broadcasted_iota(jnp.int32, (16, 128), 1)
    down = jnp.ones((16, 128), f32)
    across = jnp.ones((16, 128), f32)
    lower = jnp.zeros((16, 128), f32)

    def half(x):
        return jnp.broadcast_to(x, (8, 128))

    def full(x):
        return jnp.concatenate([x, x], axis=0)

    for base in range(0, 16, FACTOR_GROUP):
        group = range(FACTOR_GROUP)
        columns = [jnp.broadcast_to(work[:, base + i : base + i + 1], (16, 128)) for i in group]
        across_rows = [half(work[base + i : base + i + 1]) for i in group]
        corner = {
            (i, k): half(work[base + i : base + i + 1, base + k : base + k + 1])
            for i in group
            for k in range(i + 1)
        }
        scaled = []
        for i in group:
            pivot = corner[i, i]
            inverse = 1.0 / pivot
            for k in range(i + 1, FACTOR_GROUP):
                ratio = corner[k, i] * inverse
                columns[k] = columns[k] - columns[i] * full(ratio)
                across_rows[k] = across_rows[k] - across_rows[i] * ratio
                for m in range(k, FACTOR_GROUP):
                    corner[m, k] = corner[m, k] - ratio * corner[m, i]
            scaled.append(across_rows[i] * inverse)
            at = base + i
            down = jnp.where(rows == at, full(pivot), down)
            across = jnp.where(lanes == at, full(pivot), across)
            lower = jnp.where((lanes == at) & (rows >= at), columns[i], lower)
        for i in group:
            work = work - jnp.where(rows > base + i, columns[i], 0.0) * full(scaled[i])
    lower = lower / jnp.sqrt(across)
    inverse = work / jnp.sqrt(down)
    return lower[:, 0:16], inverse[:, 16:32]


def update_kernel(step, node_total, *refs):
    refs = list(refs)
    take = lambda count: [refs.pop(0) for _ in range(count)]
    (arrived,) = take(1)
    own, one, two, three = take(4)
    before, degree = (None, None) if step == 0 else take(2)
    shift_in = take(1)[0] if step > 1 else None
    (start,) = take(1) if step == 0 else (None,)
    outs = refs
    side = own[...] + one[...] + two[...] + three[...]
    height = side.shape[0] - 8
    total = arrived[0]
    for p in range(1, arrived.shape[0]):
        total = total + arrived[p]
    gram = unpack_gram(side[height : height + 8], 64) * (1.0 / node_total)
    if step == 0:
        level = side[16:17] + jnp.concatenate([total[4, 0:1], total[4, 1:2]], axis=1)
        total = from_tiles(total[0:4])
    total = total + side[0:16]
    if step == 0:
        packed, piece_out, state, degree_out, lower_out = outs
        lower, inverse = factor_and_inverse(gram[:, 0:16])
        block = start[...]
        applied = level * block - total[0:16]
        both = dot_f32(inverse, jnp.concatenate([block, applied], axis=1), ((1,), (0,)))
        degree_out[...] = jnp.broadcast_to(level, degree_out.shape)
        stack = both
        new_vectors = both[:, 0:256]
        new_applied = both[:, 256:512]
        state[...] = both
        basis = new_vectors
        lower_out[...] = lower
    else:
        if step == 1:
            packed, piece_out, state, coeff_out, lower_out, shift_out = outs
        else:
            packed, piece_out, state, coeff_out, lower_out = outs
        width = 16 * step
        coeffs = gram[:, 0:width]
        square = gram[:, width : width + 16]
        square = square - dot_f32(coeffs, coeffs, ((1,), (1,)))
        lower, inverse = factor_and_inverse(square)
        stack = before[...]
        newest = stack[width - 16 : width]
        vectors, applied = newest[:, 0:256], newest[:, 256:512]
        level = degree[0:1]
        twice = level * applied - total[0:16]
        coeff_out[...] = jnp.concatenate([coeffs, jnp.zeros((16, 128 - width), f32)], axis=1)
        if step == 1:
            shift = jnp.broadcast_to(
                jnp.sum(coeffs * eye16(), axis=(0, 1), keepdims=True) * (1.0 / 16), (8, 128)
            )
            shift_out[...] = shift
            scalar = shift[0:1, 0:1]
            moved = applied - scalar * vectors
            twice = twice - scalar * applied - scalar * moved
            coeffs = coeffs - scalar * eye16()
            applied = moved
            stack = jnp.concatenate([vectors, applied], axis=1)
        else:
            scalar = shift_in[0:1, 0:1]
            twice = twice - scalar * applied
            coeff_out[:, width - 16 : width] = coeffs[:, width - 16 : width] + scalar * eye16()
        rest = jnp.concatenate([applied, twice], axis=1) - dot_f32(coeffs, stack, ((1,), (0,)))
        both = dot_f32(inverse, rest, ((1,), (0,)))
        state[0:width] = stack
        state[width : width + 16] = both
        lower_out[...] = lower
        new_applied = both[:, 256:512]
        basis = jnp.concatenate([stack[:, 0:256], both[:, 0:256]], axis=0)
    partial = dot_f32(new_applied, jnp.concatenate([basis, new_applied], axis=0), ((1,), (1,)))
    piece_out[...] = new_applied
    if step == ITERS - 1:
        message = pack_gram(partial, 128)
        for p in range(packed.shape[0]):
            packed[p] = message
    else:
        message = jnp.concatenate([to_tiles(new_applied), pack_gram(partial)[None]], axis=0)
        for p in range(packed.shape[0]):
            packed[p] = message


def update(step, node_total, arrived, sides, state, degree, shift, start):
    size = sides[0].shape[1]
    shapes = [
        jax.ShapeDtypeStruct((8, 8, size) if step == ITERS - 1 else (16, 5, 8, 128), f32),
        jax.ShapeDtypeStruct((16, size), f32),
        jax.ShapeDtypeStruct((16 * (step + 1), 2 * size), f32),
    ]
    if step == 0:
        shapes += [jax.ShapeDtypeStruct((8, size), f32), jax.ShapeDtypeStruct((16, 16), f32)]
        extra = [start]
    else:
        shapes += [jax.ShapeDtypeStruct((16, 128), f32), jax.ShapeDtypeStruct((16, 16), f32)]
        extra = [state, degree]
        if step == 1:
            shapes.append(jax.ShapeDtypeStruct((8, 128), f32))
        else:
            extra.append(shift)
    args = [arrived, *sides, *extra]
    return pl.pallas_call(
        functools.partial(update_kernel, step, node_total),
        out_shape=tuple(shapes),
        in_specs=[VMEM] * len(args),
        out_specs=(VMEM,) * len(shapes),
        compiler_params=limits(16),
        cost_estimate=cost(400_000_000),
    )(*args)


def fold_kernel(arrived, packed):
    total = arrived[0]
    for p in range(1, arrived.shape[0]):
        total = total + arrived[p]
    for p in range(packed.shape[0]):
        packed[p] = total


def fold(arrived):
    return pl.pallas_call(
        fold_kernel,
        name="fold",
        out_shape=jax.ShapeDtypeStruct((16, 8, arrived.shape[2]), f32),
        in_specs=[VMEM],
        out_specs=VMEM,
        compiler_params=limits(8),
    )(arrived)


def last_kernel(node_total, arrived, state, shift, *refs):
    coeffs_in, lowers_in = refs[0 : ITERS - 1], refs[ITERS - 1 : 2 * ITERS - 1]
    basis_out, coeffs_out, lowers_out = refs[2 * ITERS - 1 :]
    packed = arrived[0]
    for p in range(1, arrived.shape[0]):
        packed = packed + arrived[p]
    gram = unpack_gram(packed, 128) * (1.0 / node_total)
    width = 16 * ITERS
    coeffs = gram[:, 0:width]
    square = gram[:, width : width + 16] - dot_f32(coeffs, coeffs, ((1,), (1,)))
    stack = state[...]
    rest = stack[width - 16 : width, 256:512] - dot_f32(coeffs, stack[:, 0:256], ((1,), (0,)))
    for k in range(ITERS):
        basis_out[k] = stack[16 * k : 16 * k + 16, 0:256]
        lowers_out[k] = lowers_in[k][...]
        for j in range(ITERS):
            if j > k:
                coeffs_out[k, j] = jnp.zeros((16, 16), f32)
            elif k < ITERS - 1:
                coeffs_out[k, j] = coeffs_in[k][:, 16 * j : 16 * j + 16]
            elif j < k:
                coeffs_out[k, j] = coeffs[:, 16 * j : 16 * j + 16]
            else:
                coeffs_out[k, j] = coeffs[:, 16 * j : 16 * j + 16] + shift[0:1, 0:1] * eye16()
    lower, inverse = factor_and_inverse(square)
    basis_out[ITERS] = dot_f32(inverse, rest, ((1,), (0,)))
    lowers_out[ITERS] = lower


def last(node_total, arrived, state, shift, coeffs, lowers):
    args = [arrived, state, shift, *coeffs, *lowers]
    return pl.pallas_call(
        functools.partial(last_kernel, node_total),
        name="last",
        out_shape=(
            jax.ShapeDtypeStruct((ITERS + 1, 16, arrived.shape[2]), f32),
            jax.ShapeDtypeStruct((ITERS, ITERS, 16, 16), f32),
            jax.ShapeDtypeStruct((ITERS + 1, 16, 16), f32),
        ),
        in_specs=[VMEM] * len(args),
        out_specs=(VMEM,) * 3,
        compiler_params=limits(8),
    )(*args)


def first_message_kernel(block, tiles, packed, piece, ahead, sems):
    piece_copy = pltpu.make_async_copy(block, piece, sems.at[0])
    ahead_copy = pltpu.make_async_copy(tiles.at[0, 0, pl.ds(0, AHEAD)], ahead, sems.at[1])
    piece_copy.start()
    ahead_copy.start()
    piece_copy.wait()
    for p in range(packed.shape[0]):
        packed[p] = piece[...]
    ahead_copy.wait()


def first_message(block, tiles):
    size = tiles.shape[3]
    return pl.pallas_call(
        first_message_kernel,
        name="first_message",
        out_shape=(
            jax.ShapeDtypeStruct((16, *block.shape), f32),
            pltpu.VMEM(block.shape, f32),
            pltpu.VMEM((AHEAD, size, size), f32),
        ),
        in_specs=[HBM, HBM],
        out_specs=(VMEM, VMEM, VMEM),
        scratch_shapes=[pltpu.SemaphoreType.DMA((2,))],
        compiler_params=limits(6),
    )(block, tiles)


def shifted(value, hop):
    size = lax.axis_size("grp")
    return lax.ppermute(value, "grp", [(i, (i + hop) % size) for i in range(size)])


def swapped(value):
    return lax.ppermute(value, CORE, [(0, 1), (1, 0)])


def exchanged(value, axes):
    return lax.all_to_all(value, axes, split_axis=0, concat_axis=0, tiled=True)


def body(start_block, tile_values, tile_row, tile_col, tile_count):
    grp_size = lax.axis_size("grp")
    node_total = float(start_block.shape[1] * grp_size * lax.axis_size(COL))
    HBM_SPACE = pltpu.MemorySpace.HBM

    def placed_in(space):
        index = [pltpu.with_memory_space_constraint(part, space) for part in (tile_row, tile_col)]
        return (*index, tile_count)

    first_place, place = placed_in(HBM_SPACE), placed_in(pltpu.VMEM)
    raw_block = start_block
    start_block = pltpu.with_memory_space_constraint(start_block, HBM_SPACE)
    tile_values = pltpu.with_memory_space_constraint(tile_values, pltpu.MemorySpace.HBM)
    message, piece, ahead = first_message(start_block, tile_values)
    ahead = pltpu.with_memory_space_constraint(ahead, pltpu.VMEM)
    origin = piece
    state = degree = shift = parts = None
    lowers, coeffs = [], []
    for step in range(ITERS):
        first = step == 0
        pieces = [piece]
        for hop in range(1, grp_size):
            pieces.append(shifted(raw_block if first else piece, hop))
        near = exchanged(message, ZX)
        if first:
            rows, *parts = rows_first(first_place, tile_values, ahead, pieces)
            parts = [
                pltpu.with_memory_space_constraint(part, space)
                for part, space in zip(
                    parts, (pltpu.VMEM,) * 2 + (pltpu.MemorySpace.HBM,) * 2, strict=True
                )
            ]
        else:
            rows = rows_next(place, parts, pieces)
        far = swapped(near)
        arrived = exchanged(rows, COL)
        cols = cols_product(first, place, parts, near, far)
        sides = [cols[0]]
        for hop in range(1, grp_size):
            sides.append(shifted(cols[hop], hop))
        outs = update(step, node_total, arrived, sides, state, degree, shift, origin)
        message, piece, state = outs[0:3]
        if first:
            degree = outs[3]
        else:
            coeffs.append(outs[3])
        lowers.append(outs[4])
        if step == 1:
            shift = outs[5]
    packed = fold(exchanged(message, ("col_1", "col_2")))
    packed = exchanged(packed, ("grp", "col_0"))
    return last(node_total, packed, state, shift, coeffs, lowers)


def solution(mesh):
    split_mesh = Mesh(
        mesh.devices.reshape(mesh.shape["grp"], 4, 4, 2), ("grp", "col_0", "col_1", "col_2")
    )
    placed = (
        P(None, GRP_COL),
        P("grp", COL, None, None, None),
        P("grp", COL, None),
        P("grp", COL, None),
        P("grp", COL),
    )
    return jax.shard_map(
        body,
        mesh=split_mesh,
        in_specs=placed,
        out_specs=(P(None, None, GRP_COL), P(), P()),
        check_vma=False,
    )
```
